256 devices in a mesh: trunk: 8 (over x, core), branch: 32 (over z, y).
Axes of the slice: x: 4, y: 4, z: 8, core: 2. Of those that a mesh axis runs over, the one named last changes fastest.
Arguments:
- queries: bfloat16 [8, 4096, 4096], P('trunk', 'branch'), may hold values from -160 to 160
- keys_values: bfloat16 [8, 4096, 2, 512], P('trunk', 'branch'), may hold values from -7 to 7
- out_grad: bfloat16 [8, 4096, 4096], P('trunk', 'branch'), may hold values from -6 to 6
- trunk_kv: bfloat16 [8, 32, 2, 16, 512], P('trunk', 'branch'), may hold values from -6 to 6
- branch_of: int32 [8, 4096], P('trunk', 'branch'), may hold values from 0 to 63, never falling along the last dimension, each value on 1 to 128 neighbouring positions
- branch_reach: int32 [8, 64], P('trunk'), may hold values from 1 to 8
- ancestors: int32 [8, 32, 8], P('trunk', 'branch'), may hold values from 0 to 31
Outputs:
- attended: bfloat16 [8, 4096, 4096], P('trunk', 'branch')
- query_grad: bfloat16 [8, 4096, 4096], P('trunk', 'branch')
- kv_grad: float32 [8, 4096, 2, 512], P('trunk', 'branch')
- trunk_grad: float32 [8, 32, 2, 16, 512], P('trunk', 'branch')
The draws below stay inside these ranges and needn't reach their ends.
Inputs may be any that keep to these rules, and one draw needn't show every extreme that they name: `branch_of`: ids never fall along a row; each branch covers 1 to 128 consecutive tokens. `ancestors`: entry d names the branch index of the device at trunk index d that holds the segment read at depth d.
All inputs are finite; a program needn't handle non-finite values.
Results may differ from the reference program's by a relative error of at most 0.005.
Values may be sent and summed in bfloat16 or wider, within the bound.
A program may use at most 128 MiB of HBM per device.

```python
import math
import jax
import jax.numpy as jnp
import numpy as np
from jax import lax

HQ = 32
KVH = 4
DH = 128
Q_DEV = 128
SEG_LEN = 16
DEPTHS = 8
S_ROW = 4096
BRANCHES = 64
N_TRUNK = 8
N_BRANCH = 32


def shared_fields(key):
    base = jax.random.fold_in(key, 91)
    first_key, second_key, third_key = jax.random.split(base, 3)
    width = KVH * DH
    key_field = jnp.clip(jax.random.normal(first_key, (N_TRUNK, S_ROW, width), jnp.float32), -6.0, 6.0)
    value_field = jnp.clip(jax.random.normal(second_key, (N_TRUNK, S_ROW, width), jnp.float32), -6.0, 6.0)
    query_field = jnp.clip(jax.random.normal(third_key, (N_TRUNK, S_ROW, HQ * DH), jnp.float32), -6.0, 6.0)
    return (query_field, jnp.stack([key_field, value_field], axis=2))


def draw_queries(key, part):
    return shared_fields(key)[0].astype(jnp.bfloat16)


def draw_keys_values(key, part):
    return shared_fields(key)[1].astype(jnp.bfloat16)


def touch_ends(drawn, stream_key, smallest, high):
    longest = drawn.shape.index(max(drawn.shape))
    spots = []
    for shift in (0, 1):
        where = [jax.random.randint(jax.random.fold_in(stream_key, axis), (), 0, length) for axis, length in enumerate(drawn.shape)]
        where[longest] = (where[longest] + shift) % drawn.shape[longest]
        spots.append(tuple(where))
    return drawn.at[spots[0]].set(smallest).at[spots[1]].set(high)


def block_scale(stream_key, dims, cuts, low, top_value):
    gain = 1.0
    for axis_at, shards_of in cuts:
        steps = jax.random.uniform(jax.random.fold_in(jax.random.fold_in(stream_key, 6), axis_at), (shards_of,), jnp.float32, low / len(cuts), top_value / len(cuts))
        gain = gain * jnp.repeat(jnp.exp(steps), dims[axis_at] // shards_of).reshape((-1,) + (1,) * (len(dims) - 1 - axis_at))
    return gain


def rank_table(number_of, slope):
    portions = [(1 << 20) // math.isqrt(grade ** slope) + 1 for grade in range(1, number_of + 1)]
    scale = 1 + sum(portions) // (1 << 30)
    return np.cumsum(np.array([max(1, weight // scale) for weight in portions]))


def skewed_ids(key, extent, number_of, lean):
    table = rank_table(number_of, lean)
    lot = jax.random.randint(jax.random.fold_in(key, 1), extent, 0, int(table[number_of - 1]))
    grade = jnp.searchsorted(jnp.asarray(table, jnp.int32), lot, side="right")
    return jax.random.permutation(jax.random.fold_in(key, 2), number_of)[grade].astype(jnp.int32)


def length_profile(count, total, most, skew):
    weights = [(1 << 20) // math.isqrt(rank ** skew) + 1 for rank in range(2, count + 1)]
    surplus, counts = total - most - (count - 1), [1] * (count - 1)
    while surplus > 0:
        free = [i for i in range(count - 1) if counts[i] < most]
        pool, left = sum([weights[i] for i in free]), surplus
        for i in free:
            addition = min(most - counts[i], max(1, left * weights[i] // pool), surplus)
            counts[i] = counts[i] + addition
            surplus = surplus - addition
    return np.array([most] + counts)


def uneven_parts(stream_key, number_of, total, limit, slope):
    if number_of == 2:
        one = jax.random.randint(stream_key, (), max(1, total - limit), min(limit, total - 1) + 1)
        return jnp.stack([one, total - one])
    sizes = jnp.asarray(length_profile(number_of, total, limit, slope), jnp.int32)
    pairs = (number_of - 1) // 2
    donor, receiver = sizes[1:1 + 2 * pairs:2], sizes[2:2 + 2 * pairs:2]
    margin = jnp.minimum(donor - 1, limit - receiver)
    moved = jax.random.randint(jax.random.fold_in(stream_key, 1), (pairs,), 0, 1 << 20) % (margin + 1)
    sizes = sizes.at[1:1 + 2 * pairs:2].set(donor - moved).at[2:2 + 2 * pairs:2].set(receiver + moved)
    return sizes[jax.random.permutation(jax.random.fold_in(stream_key, 2), number_of)]


def centred(stream_key, extent, scale, limit, cuts=(), held_as=jnp.bfloat16):
    drawn = scale * jax.random.normal(stream_key, extent, jnp.float32)
    if cuts:
        drawn = drawn * block_scale(stream_key, extent, cuts, -0.22, 0.18)
    return jnp.clip(drawn, -limit, limit).astype(held_as)


def setup_inputs(seed: int = 0) -> dict:
    seeds = jax.random.split(jax.random.key(seed), 8)
    return {
        "queries": draw_queries(jax.random.fold_in(seeds[7], 71), 0),
        "keys_values": draw_keys_values(jax.random.fold_in(seeds[7], 71), 0),
        "out_grad": centred(seeds[2], (N_TRUNK, S_ROW, HQ * DH), 1.0, 6.0, ((0, 8), (1, 32))),
        "trunk_kv": centred(seeds[3], (DEPTHS, N_BRANCH, 2, SEG_LEN, KVH * DH), 1.0, 6.0, ((0, 8), (1, 32))),
        "branch_of": jax.vmap(lambda own: jnp.searchsorted(jnp.cumsum(uneven_parts(own, BRANCHES, S_ROW, Q_DEV, 2)), jnp.arange(S_ROW), side="right"))(jax.random.split(seeds[4], N_TRUNK)).reshape((N_TRUNK, S_ROW)).astype(jnp.int32),
        "branch_reach": touch_ends(jax.random.randint(seeds[5], (N_TRUNK, BRANCHES), 1, DEPTHS + 1), jax.random.fold_in(seeds[5], 1), 1, DEPTHS).astype(jnp.int32),
        "ancestors": touch_ends(skewed_ids(seeds[6], (N_TRUNK, N_BRANCH, DEPTHS), N_BRANCH, 2), jax.random.fold_in(seeds[6], 3), 0, N_BRANCH - 1).astype(jnp.int32),
    }


def build_allowed(tags, earlier_tags, reach_rows, seg_len, depth_count):
    trunk_depth = jnp.arange(depth_count * seg_len, dtype=jnp.int32) // seg_len
    trunk_ok = trunk_depth[None, :] < reach_rows[:, None]
    earlier_ok = earlier_tags[None, :] == tags[:, None]
    position = jnp.arange(tags.shape[0], dtype=jnp.int32)
    own_ok = (tags[None, :] == tags[:, None]) & (position[None, :] <= position[:, None])
    return jnp.concatenate([trunk_ok, earlier_ok, own_ok], axis=1)

def attend_block(query_rows, grad_rows, key_rows, value_rows, allowed):
    head_scale = 1.0 / math.sqrt(DH)
    group = HQ // KVH
    n_rows = query_rows.shape[0]
    outputs, query_grads, key_grads, value_grads = ([], [], [], [])
    for head_group in range(KVH):
        query_part = query_rows[:, head_group * group * DH:(head_group + 1) * group * DH].reshape(n_rows, group, DH).astype(jnp.float32)
        grad_part = grad_rows[:, head_group * group * DH:(head_group + 1) * group * DH].reshape(n_rows, group, DH).astype(jnp.float32)
        key_part = key_rows[:, head_group * DH:(head_group + 1) * DH].astype(jnp.float32)
        value_part = value_rows[:, head_group * DH:(head_group + 1) * DH].astype(jnp.float32)
        scores = jnp.einsum('qrd,kd->rqk', query_part, key_part) * head_scale
        masked = jnp.where(allowed[None], scores, -1e+30)
        highest = lax.optimization_barrier(jnp.max(masked, axis=-1, keepdims=True))
        expo = jnp.exp(masked - highest)
        weights = expo / lax.optimization_barrier(jnp.sum(expo, axis=-1, keepdims=True))
        weights_bf = weights.astype(jnp.bfloat16).astype(jnp.float32)
        output = jnp.einsum('rqk,kd->qrd', weights_bf, value_part).reshape(n_rows, group * DH)
        grad_weights = jnp.einsum('qrd,kd->rqk', grad_part, value_part)
        row_mean = lax.optimization_barrier(jnp.sum(weights * grad_weights, axis=-1, keepdims=True))
        score_grad = (weights * (grad_weights - row_mean)).astype(jnp.bfloat16).astype(jnp.float32)
        outputs.append(output)
        query_grads.append((jnp.einsum('rqk,kd->qrd', score_grad, key_part) * head_scale).reshape(n_rows, group * DH))
        key_grads.append(jnp.einsum('rqk,qrd->kd', score_grad, query_part) * head_scale)
        value_grads.append(jnp.einsum('rqk,qrd->kd', weights_bf, grad_part))
    attended = jnp.concatenate(outputs, axis=1).astype(jnp.bfloat16)
    query_grad = jnp.concatenate(query_grads, axis=1).astype(jnp.bfloat16)
    return (attended, query_grad, jnp.concatenate(key_grads, axis=1), jnp.concatenate(value_grads, axis=1))

def reference(queries, keys_values, out_grad, trunk_kv, branch_of, branch_reach, ancestors):
    width = KVH * DH
    depth_index = jnp.arange(DEPTHS, dtype=jnp.int32)
    trunk_len = DEPTHS * SEG_LEN
    zero_index = jnp.zeros((), jnp.int32)

    def one_block(carry, block_index):
        trunk_acc, branch_acc = carry
        row = (block_index // N_BRANCH).astype(jnp.int32)
        column = (block_index % N_BRANCH).astype(jnp.int32)
        first_row = (column * Q_DEV).astype(jnp.int32)
        has_earlier = column > 0
        earlier_first = jnp.maximum(first_row - Q_DEV, 0).astype(jnp.int32)
        query_rows = lax.dynamic_slice(queries, (row, first_row, zero_index), (1, Q_DEV, HQ * DH))[0]
        grad_rows = lax.dynamic_slice(out_grad, (row, first_row, zero_index), (1, Q_DEV, HQ * DH))[0]
        own_kv = lax.dynamic_slice(keys_values, (row, first_row, zero_index, zero_index), (1, Q_DEV, 2, width))[0]
        earlier_kv = lax.dynamic_slice(keys_values, (row, earlier_first, zero_index, zero_index), (1, Q_DEV, 2, width))[0]
        earlier_kv = jnp.where(has_earlier, earlier_kv, jnp.zeros_like(earlier_kv))
        branch_ids = lax.dynamic_slice(branch_of, (row, first_row), (1, Q_DEV))[0]
        earlier_ids = lax.dynamic_slice(branch_of, (row, earlier_first), (1, Q_DEV))[0]
        tags = branch_ids + 1
        earlier_tags = jnp.where(has_earlier, earlier_ids + 1, jnp.zeros_like(earlier_ids))
        reach_table = lax.dynamic_slice(branch_reach, (row, zero_index), (1, BRANCHES))[0]
        branch_index = jnp.arange(BRANCHES, dtype=jnp.int32)
        reach_rows = lax.optimization_barrier(jnp.sum(jnp.where(branch_ids[:, None] == branch_index[None, :], reach_table[None, :], 0), axis=1)).astype(jnp.int32)
        owners = lax.dynamic_slice(ancestors, (row, column, zero_index), (1, 1, DEPTHS))[0, 0]
        fetched = trunk_kv[depth_index, owners]
        key_rows = jnp.concatenate([fetched[:, 0].reshape(trunk_len, width), earlier_kv[:, 0], own_kv[:, 0]], axis=0)
        value_rows = jnp.concatenate([fetched[:, 1].reshape(trunk_len, width), earlier_kv[:, 1], own_kv[:, 1]], axis=0)
        allowed = build_allowed(tags, earlier_tags, reach_rows, SEG_LEN, DEPTHS)
        attended, query_grad, key_grad, value_grad = attend_block(query_rows, grad_rows, key_rows, value_rows, allowed)
        trunk_part = jnp.stack([key_grad[:trunk_len].reshape(DEPTHS, SEG_LEN, width), value_grad[:trunk_len].reshape(DEPTHS, SEG_LEN, width)], axis=1)
        trunk_acc = trunk_acc.at[depth_index, owners].add(trunk_part)
        earlier_part = jnp.stack([key_grad[trunk_len:trunk_len + Q_DEV], value_grad[trunk_len:trunk_len + Q_DEV]], axis=1)
        earlier_part = jnp.where(has_earlier, earlier_part, jnp.zeros_like(earlier_part))
        own_part = jnp.stack([key_grad[trunk_len + Q_DEV:], value_grad[trunk_len + Q_DEV:]], axis=1)
        current = lax.dynamic_slice(branch_acc, (row, earlier_first, zero_index, zero_index), (1, Q_DEV, 2, width))
        branch_acc = lax.dynamic_update_slice(branch_acc, current + earlier_part[None], (row, earlier_first, zero_index, zero_index))
        current = lax.dynamic_slice(branch_acc, (row, first_row, zero_index, zero_index), (1, Q_DEV, 2, width))
        branch_acc = lax.dynamic_update_slice(branch_acc, current + own_part[None], (row, first_row, zero_index, zero_index))
        return ((trunk_acc, branch_acc), (attended, query_grad))
    start_carry = (jnp.zeros(trunk_kv.shape, jnp.float32), jnp.zeros(keys_values.shape, jnp.float32))
    (trunk_acc, branch_acc), (attended, query_grad) = lax.scan(one_block, start_carry, jnp.arange(N_TRUNK * N_BRANCH, dtype=jnp.int32))
    attended = attended.reshape(N_TRUNK, S_ROW, HQ * DH)
    query_grad = query_grad.reshape(N_TRUNK, S_ROW, HQ * DH)
    return (attended, query_grad, branch_acc, trunk_acc)
```

```python
import functools
import math

import jax
import jax.numpy as jnp
from jax import lax
from jax.experimental import pallas as pl
from jax.experimental.pallas import tpu as pltpu
from jax.sharding import PartitionSpec as P

KVH = 4
DH = 128
NEG = -1e30
LOG2E = math.log2(math.e)
MESH = pl.DeviceIdType.MESH


def attention_kernel(
    tags_ref, earlier_tags_ref, reach_ref, q_ref, g_ref, trunk_ref, earlier_ref, own_ref,
    att_ref, qg_ref, dtrunk_ref, dearlier_ref, down_ref, bias, weights, grads,
):
    rows = q_ref.shape[0]
    group = q_ref.shape[1] // DH
    depths, seg_len = trunk_ref.shape[0], trunk_ref.shape[3]
    trunk_len = depths * seg_len
    keys = trunk_len + 2 * rows
    scale = 1.0 / math.sqrt(DH)

    @pl.when(pl.program_id(0) == 0)
    def _():
        row_tags = tags_ref[...]
        squares = jnp.broadcast_to(row_tags, (rows, rows))
        column_tags = squares.T
        earlier_column = jnp.broadcast_to(earlier_tags_ref[...], (rows, rows)).T
        depth = lax.broadcasted_iota(jnp.int32, (trunk_len, rows), 0) // seg_len
        position = lax.broadcasted_iota(jnp.int32, (rows, rows), 0)
        query = lax.broadcasted_iota(jnp.int32, (rows, rows), 1)
        bias[:trunk_len] = jnp.where(depth < reach_ref[...], 0.0, NEG)
        bias[trunk_len : trunk_len + rows] = jnp.where(earlier_column == squares, 0.0, NEG)
        bias[trunk_len + rows :] = jnp.where(
            (column_tags == squares) & (position <= query), 0.0, NEG
        )

    def stacked(part):
        return jnp.concatenate(
            [trunk_ref[:, 0, part].reshape(trunk_len, DH), earlier_ref[part], own_ref[part]], axis=0
        )

    key_rows, value_rows = stacked(0), stacked(1)
    key_cols, value_cols = key_rows.T, value_rows.T
    allowed = bias[...]
    allowed = jnp.concatenate([allowed, allowed], axis=1)
    nt = (((1,), (1,)), ((), ()))

    def heads(ref, first):
        return jnp.concatenate(
            [ref[:, (first + i) * DH : (first + i + 1) * DH] for i in range(2)], axis=0
        )

    for first in range(0, group, 2):
        q2, g2 = heads(q_ref, first), heads(g_ref, first)
        scores = lax.dot_general(key_rows, q2, nt, preferred_element_type=jnp.float32) + allowed
        highest = jnp.max(scores, axis=0, keepdims=True)
        expo = jnp.exp2((scores - highest) * (scale * LOG2E))
        w = expo * (1.0 / jnp.sum(expo, axis=0, keepdims=True))
        w_bf = w.astype(jnp.bfloat16)
        gw = lax.dot_general(value_rows, g2, nt, preferred_element_type=jnp.float32)
        row_mean = jnp.sum(w * gw, axis=0, keepdims=True)
        sg = (w * (gw - row_mean)).astype(jnp.bfloat16)
        columns = slice(first * rows, (first + 2) * rows)
        weights[:, columns] = w_bf
        grads[:, columns] = sg
        out = jnp.dot(value_cols, w_bf, preferred_element_type=jnp.float32)
        dq = jnp.dot(key_cols, sg, preferred_element_type=jnp.float32) * scale
        for i in range(2):
            at = slice((first + i) * DH, (first + i + 1) * DH)
            part = slice(i * rows, (i + 1) * rows)
            att_ref[:, at] = out[:, part].T.astype(jnp.bfloat16)
            qg_ref[:, at] = dq[:, part].T.astype(jnp.bfloat16)

    def all_heads(ref):
        return jnp.concatenate([ref[:, i * DH : (i + 1) * DH] for i in range(group)], axis=0)

    dk = jnp.dot(grads[...], all_heads(q_ref), preferred_element_type=jnp.float32) * scale
    dv = jnp.dot(weights[...], all_heads(g_ref), preferred_element_type=jnp.float32)
    for part, grad in enumerate((dk, dv)):
        dtrunk_ref[:, 0, part] = (
            grad[:trunk_len].reshape(depths, seg_len, DH).astype(dtrunk_ref.dtype)
        )
        dearlier_ref[part] = grad[trunk_len : trunk_len + rows].astype(dearlier_ref.dtype)
        down_ref[part] = grad[trunk_len + rows :]


def attention(tags, earlier_tags, reach, q, g, trunk, earlier, own):
    rows, width = q.shape
    depths, heads, _, seg_len, _ = trunk.shape
    keys = depths * seg_len + 2 * rows
    wide = width // heads
    small = pl.BlockSpec((1, rows), lambda i: (0, 0))
    tall = pl.BlockSpec((rows, wide), lambda i: (0, i))
    segs = pl.BlockSpec((depths, 1, 2, seg_len, DH), lambda i: (0, i, 0, 0, 0))
    kv = pl.BlockSpec((2, rows, DH), lambda i: (0, 0, i))
    return pl.pallas_call(
        attention_kernel,
        grid=(heads,),
        in_specs=[small, small, small, tall, tall, segs, kv, kv],
        out_specs=[tall, tall, segs, kv, kv],
        out_shape=[
            jax.ShapeDtypeStruct(q.shape, jnp.bfloat16),
            jax.ShapeDtypeStruct(q.shape, jnp.bfloat16),
            jax.ShapeDtypeStruct(trunk.shape, jnp.bfloat16),
            jax.ShapeDtypeStruct(earlier.shape, jnp.bfloat16),
            jax.ShapeDtypeStruct(own.shape, jnp.float32),
        ],
        scratch_shapes=[
            pltpu.VMEM((keys, rows), jnp.float32),
            pltpu.VMEM((keys, wide), jnp.bfloat16),
            pltpu.VMEM((keys, wide), jnp.bfloat16),
        ],
        compiler_params=pltpu.CompilerParams(dimension_semantics=("arbitrary",)),
        cost_estimate=pl.CostEstimate(
            flops=12 * width * rows * keys, bytes_accessed=8 * rows * width, transcendentals=width * keys
        ),
        name="attention",
    )(tags, earlier_tags, reach, q, g, trunk, earlier, own)


def places():
    trunk, branch = lax.axis_index("trunk"), lax.axis_index("branch")
    return trunk, branch, branch // KVH, lax.rem(branch, KVH)


def served(index, trunk, z):
    return index // KVH, z * KVH + lax.rem(index, KVH)


def meet(trunk, branch, z, n_trunk, n_branch):
    barrier = pltpu.get_barrier_semaphore()

    def greet_branch(i, carry):
        pl.semaphore_signal(
            barrier, inc=1, device_id=(trunk, lax.rem(branch + i, n_branch)), device_id_type=MESH
        )
        return carry

    def greet_trunk(i, carry):
        pl.semaphore_signal(
            barrier,
            inc=1,
            device_id=(
                lax.rem(trunk + 1 + i // KVH, n_trunk),
                z * KVH + lax.rem(branch + lax.rem(i, KVH), KVH),
            ),
            device_id_type=MESH,
        )
        return carry

    lax.fori_loop(1, n_branch, greet_branch, 0)
    lax.fori_loop(0, (n_trunk - 1) * KVH, greet_trunk, 0)
    pl.semaphore_wait(barrier, n_branch - 1 + (n_trunk - 1) * KVH)


def send(source, target, send_sem, recv_sem, trunk, branch):
    pltpu.make_async_remote_copy(
        src_ref=source,
        dst_ref=target,
        send_sem=send_sem,
        recv_sem=recv_sem,
        device_id=(trunk, branch),
        device_id_type=MESH,
    ).start()


def arrived(ref, sem):
    pltpu.make_async_copy(ref, ref, sem).wait()


def to_branch(n_branch, trunk, branch, source, target, send_sem, recv_sem):
    def step(i, carry):
        other = lax.rem(branch + i, n_branch)
        send(source(other), target, send_sem, recv_sem, trunk, other)
        return carry

    lax.fori_loop(1, n_branch, step, 0)


def to_served(n_trunk, trunk, branch, z, y, source, target, send_sem, recv_sem):
    def step(i, carry):
        turn = i + 1
        t = lax.rem(trunk + turn // KVH, n_trunk)
        other = lax.rem(y + lax.rem(turn, KVH), KVH)
        send(source(t, other), target, send_sem, recv_sem, t, z * KVH + other)
        return carry

    lax.fori_loop(0, n_trunk * KVH - 1, step, 0)


def fetch_kernel(
    n_trunk, n_branch, segment_ref, asked_ref, own_ref, tags_ref,
    fetched_ref, earlier_ref, earlier_tags_ref, requests_ref,
    held, asked, wanted, staged, got, before, before_tags,
    send_sems, recv_sems, local_sems,
):
    trunk, branch, z, y = places()
    meet(trunk, branch, z, n_trunk, n_branch)
    me = trunk * KVH + y
    to_served(
        n_trunk, trunk, branch, z, y, lambda t, o: asked_ref, asked.at[me], send_sems.at[0], recv_sems.at[0]
    )
    mine = pltpu.make_async_copy(asked_ref, asked.at[me], recv_sems.at[0])
    mine.start()

    def head(at):
        return segment_ref.at[:, :, pl.ds(pl.multiple_of(at * DH, DH), DH)]

    to_branch(
        n_branch, trunk, branch, lambda b: head(lax.rem(b, KVH)), held.at[branch], send_sems.at[1], recv_sems.at[1]
    )
    pltpu.make_async_copy(head(y), held.at[branch], recv_sems.at[1]).start()
    after = lax.rem(branch + 1, n_branch)
    send(own_ref, before, send_sems.at[2], recv_sems.at[2], trunk, after)
    send(tags_ref, before_tags, send_sems.at[3], recv_sems.at[3], trunk, after)

    arrived(asked, recv_sems.at[0])
    local = pltpu.make_async_copy(asked, wanted, local_sems.at[0])
    local.start()
    local.wait()
    arrived(held, recv_sems.at[1])

    def pick(i, carry):
        staged[i] = held[wanted[i, 0, trunk]]
        return carry

    lax.fori_loop(0, n_trunk * KVH, pick, 0)
    to_served(
        n_trunk, trunk, branch, z, y, lambda t, o: staged.at[t * KVH + o], got.at[me], send_sems.at[4], recv_sems.at[4]
    )
    pltpu.make_async_copy(staged.at[me], got.at[me], recv_sems.at[4]).start()
    requests_ref[...] = asked[...]
    arrived(before, recv_sems.at[2])
    arrived(before_tags, recv_sems.at[3])
    earlier_ref[...] = before[...]
    earlier_tags_ref[...] = jnp.where(branch > 0, before_tags[...], 0)
    arrived(got, recv_sems.at[4])
    fetched_ref[...] = got[...]
    others = n_trunk * KVH - 1
    arrived(asked.at[pl.ds(0, others)], send_sems.at[0])
    arrived(held.at[pl.ds(0, n_branch - 1)], send_sems.at[1])
    arrived(own_ref, send_sems.at[2])
    arrived(tags_ref, send_sems.at[3])
    arrived(staged.at[pl.ds(0, others)], send_sems.at[4])


def fetch(n_trunk, n_branch, segment, asked, own, tags):
    n_served = n_trunk * KVH
    seg_len = segment.shape[1]
    piece = (2, seg_len, DH)
    vmem = pl.BlockSpec(memory_space=pltpu.VMEM)
    return pl.pallas_call(
        functools.partial(fetch_kernel, n_trunk, n_branch),
        in_specs=[vmem] * 4,
        out_specs=[vmem] * 4,
        out_shape=[
            jax.ShapeDtypeStruct((n_served, *piece), jnp.bfloat16),
            jax.ShapeDtypeStruct(own.shape, jnp.bfloat16),
            jax.ShapeDtypeStruct(tags.shape, jnp.int32),
            jax.ShapeDtypeStruct((n_served, *asked.shape), jnp.int32),
        ],
        scratch_shapes=[
            pltpu.VMEM((n_branch, *piece), jnp.bfloat16),
            pltpu.VMEM((n_served, *asked.shape), jnp.int32),
            pltpu.SMEM((n_served, *asked.shape), jnp.int32),
            pltpu.VMEM((n_served, *piece), jnp.bfloat16),
            pltpu.VMEM((n_served, *piece), jnp.bfloat16),
            pltpu.VMEM(own.shape, jnp.bfloat16),
            pltpu.VMEM(tags.shape, jnp.int32),
            pltpu.SemaphoreType.DMA((5,)),
            pltpu.SemaphoreType.DMA((5,)),
            pltpu.SemaphoreType.DMA((1,)),
        ],
        compiler_params=pltpu.CompilerParams(collective_id=0, has_side_effects=True),
        name="fetch",
    )(segment, asked, own, tags)


def return_kernel(
    n_trunk, n_branch, requests_ref, dtrunk_ref, dearlier_ref,
    trunk_grad_ref, from_next_ref,
    came, summed, sums, after_grad, send_sems, recv_sems,
):
    trunk, branch, z, y = places()
    meet(trunk, branch, z, n_trunk, n_branch)
    me = trunk * KVH + y
    to_served(
        n_trunk, trunk, branch, z, y, lambda t, o: dtrunk_ref.at[t * KVH + o], came.at[me], send_sems.at[0], recv_sems.at[0]
    )
    pltpu.make_async_copy(dtrunk_ref.at[me], came.at[me], recv_sems.at[0]).start()
    send(
        dearlier_ref, after_grad, send_sems.at[1], recv_sems.at[1], trunk, lax.rem(branch + n_branch - 1, n_branch)
    )
    arrived(came, recv_sems.at[0])

    def add_up(owner, carry):
        total = jnp.zeros(came.shape[1:], jnp.float32)
        for i in range(n_trunk * KVH):
            hit = jnp.where(requests_ref[i, 0, trunk] == owner, 1.0, 0.0)
            total = total + came[i].astype(jnp.float32) * hit
        summed[owner] = total.astype(jnp.bfloat16)
        return carry

    lax.fori_loop(0, n_branch, add_up, 0)
    to_branch(
        n_branch, trunk, branch, lambda b: summed.at[b], sums.at[branch], send_sems.at[2], recv_sems.at[2]
    )
    pltpu.make_async_copy(summed.at[branch], sums.at[branch], recv_sems.at[2]).start()
    arrived(after_grad, recv_sems.at[1])
    from_next_ref[...] = after_grad[...]
    arrived(sums, recv_sems.at[2])
    for head in range(KVH):
        total = sums[head].astype(jnp.float32)
        for i in range(1, n_branch // KVH):
            total = total + sums[i * KVH + head].astype(jnp.float32)
        trunk_grad_ref[:, :, head * DH : (head + 1) * DH] = total
    arrived(came.at[pl.ds(0, n_trunk * KVH - 1)], send_sems.at[0])
    arrived(dearlier_ref, send_sems.at[1])
    arrived(sums.at[pl.ds(0, n_branch - 1)], send_sems.at[2])


def give_back(n_trunk, n_branch, requests, dtrunk, dearlier):
    vmem = pl.BlockSpec(memory_space=pltpu.VMEM)
    piece = dtrunk.shape[1:]
    return pl.pallas_call(
        functools.partial(return_kernel, n_trunk, n_branch),
        in_specs=[pl.BlockSpec(memory_space=pltpu.SMEM), vmem, vmem],
        out_specs=[vmem] * 2,
        out_shape=[
            jax.ShapeDtypeStruct((*piece[:2], KVH * DH), jnp.float32),
            jax.ShapeDtypeStruct(dearlier.shape, jnp.bfloat16),
        ],
        scratch_shapes=[
            pltpu.VMEM(dtrunk.shape, jnp.bfloat16),
            pltpu.VMEM((n_branch, *piece), jnp.bfloat16),
            pltpu.VMEM((n_branch, *piece), jnp.bfloat16),
            pltpu.VMEM(dearlier.shape, jnp.bfloat16),
            pltpu.SemaphoreType.DMA((3,)),
            pltpu.SemaphoreType.DMA((3,)),
        ],
        compiler_params=pltpu.CompilerParams(collective_id=1, has_side_effects=True),
        name="give_back",
    )(requests, dtrunk, dearlier)


def on_device(queries, keys_values, out_grad, trunk_kv, branch_of, branch_reach, ancestors):
    n_trunk, n_branch = lax.axis_size("trunk"), lax.axis_size("branch")
    seg_len = trunk_kv.shape[3]
    own = jnp.moveaxis(keys_values[0], 1, 0)
    branch_ids = branch_of[0]
    tags = (branch_ids + 1)[None]
    asked = jnp.pad(ancestors[0], ((0, 0), (0, DH - n_trunk)))
    fetched, earlier, earlier_tags, requests = fetch(
        n_trunk, n_branch, trunk_kv[0, 0], asked, own, tags
    )
    reach_table = branch_reach[0]
    branch_index = jnp.arange(reach_table.shape[0], dtype=jnp.int32)
    reach_rows = jnp.sum(
        jnp.where(branch_ids[:, None] == branch_index[None, :], reach_table[None, :], 0), axis=1
    )
    attended, query_grad, dtrunk, dearlier, down = attention(
        tags,
        earlier_tags,
        reach_rows[None],
        queries[0],
        out_grad[0],
        fetched.reshape(n_trunk, KVH, 2, seg_len, DH),
        earlier,
        own,
    )
    trunk_grad, from_next = give_back(
        n_trunk, n_branch, requests, dtrunk.reshape(fetched.shape), dearlier
    )
    kv_grad = jnp.moveaxis(down + from_next.astype(jnp.float32), 0, 1)
    return (attended[None], query_grad[None], kv_grad[None], trunk_grad[None, None])


def solution(mesh):
    return jax.shard_map(
        on_device,
        mesh=mesh,
        in_specs=(
            P("trunk", "branch", None),
            P("trunk", "branch", None, None),
            P("trunk", "branch", None),
            P("trunk", "branch", None, None, None),
            P("trunk", "branch"),
            P("trunk", None),
            P("trunk", "branch", None),
        ),
        out_specs=(
            P("trunk", "branch", None),
            P("trunk", "branch", None),
            P("trunk", "branch", None, None),
            P("trunk", "branch", None, None, None),
        ),
        check_vma=False,
    )
```

```python
import functools
import math

import jax
import jax.numpy as jnp
from jax import lax
from jax.experimental import pallas as pl
from jax.experimental.pallas import tpu as pltpu
from jax.sharding import PartitionSpec as P

KVH = 4
DH = 128
NEG = -1e30
SCALE = 1.0 / math.sqrt(DH)
EXP2_SCALE = SCALE * math.log2(math.e)
MESH = pl.DeviceIdType.MESH
NT = (((1,), (1,)), ((), ()))
HEADS_BEFORE_SUMS = 3


def dot(a, b):
    return jnp.dot(a, b, preferred_element_type=jnp.float32)


def dot_nt(a, b):
    return lax.dot_general(a, b, NT, preferred_element_type=jnp.float32)


def signal(semaphore, trunk, branch):
    pl.semaphore_signal(semaphore, inc=1, device_id=(trunk, branch), device_id_type=MESH)


def send(source, target, send_sem, recv_sem, trunk, branch):
    pltpu.make_async_remote_copy(
        src_ref=source,
        dst_ref=target,
        send_sem=send_sem,
        recv_sem=recv_sem,
        device_id=(trunk, branch),
        device_id_type=MESH,
    ).start()


def arrived(ref, sem):
    pltpu.make_async_copy(ref, ref, sem).wait()


def loop(first, last, body):
    def step(i, carry):
        body(i)
        return carry

    lax.fori_loop(first, last, step, 0)


def columns(head):
    return pl.ds(pl.multiple_of(head * DH, DH), DH)


def kernel(
    n_trunk, n_branch,
    q_hbm, g_hbm, own_ref, segment_ref, asked_ref, tags_ref, reach_ref,
    att_hbm, qg_hbm, kv_grad_ref, trunk_grad_ref,
    q, g, held, asked, wanted, staged, got, before, before_tags, bias, early, early_gw, stats,
    weights, grads, att, qg, dtrunk, dbefore, down, came, summed, sums, after_grad,
    load_sems, store_sems, local_sem, send_sems, recv_sems,
):
    trunk, branch = lax.axis_index("trunk"), lax.axis_index("branch")
    z, y = branch // KVH, lax.rem(branch, KVH)
    me = trunk * KVH + y
    n_served = n_trunk * KVH
    heads = q.shape[0]
    pairs = heads // 2
    per_group = pairs // KVH
    rows = q.shape[1]
    trunk_len = n_trunk * segment_ref.shape[1]
    after = lax.rem(branch + 1, n_branch)
    previous = lax.rem(branch + n_branch - 1, n_branch)

    barrier = pltpu.get_barrier_semaphore()
    loop(1, n_branch, lambda i: signal(barrier, trunk, lax.rem(branch + i, n_branch)))
    loop(
        0,
        (n_trunk - 1) * KVH,
        lambda i: signal(
            barrier, lax.rem(trunk + 1 + i // KVH, n_trunk), z * KVH + lax.rem(branch + lax.rem(i, KVH), KVH)
        ),
    )

    def load(i):
        pltpu.make_async_copy(q_hbm.at[:, columns(i)], q.at[i], load_sems.at[0]).start()
        pltpu.make_async_copy(g_hbm.at[:, columns(i)], g.at[i], load_sems.at[1]).start()

    loop(0, heads, load)

    squares = jnp.broadcast_to(tags_ref[...], (rows, rows))
    position = lax.broadcasted_iota(jnp.int32, (rows, rows), 0)
    query = lax.broadcasted_iota(jnp.int32, (rows, rows), 1)
    bias[2] = jnp.where((squares.T == squares) & (position <= query), 0.0, NEG)
    branches = reach_ref.shape[1]
    reach_column = jnp.broadcast_to(reach_ref[...].astype(jnp.float32), (branches, branches)).T
    branch_index = lax.broadcasted_iota(jnp.int32, (branches, rows), 0)
    reach = jnp.sum(
        jnp.where(branch_index == tags_ref[...], reach_column[:, :1], 0.0), axis=0, keepdims=True
    )
    depth = lax.broadcasted_iota(jnp.int32, (trunk_len, rows), 0) // segment_ref.shape[1]
    bias[0] = jnp.where(depth.astype(jnp.float32) < reach, 0.0, NEG)

    pl.semaphore_wait(barrier, n_branch - 1 + (n_trunk - 1) * KVH)

    def to_served(source, target, send_sem, recv_sem):
        def step(i):
            t = lax.rem(trunk + i // KVH, n_trunk)
            other = lax.rem(y + lax.rem(i, KVH), KVH)
            send(source(t, other), target, send_sem, recv_sem, t, z * KVH + other)

        loop(1, n_served, step)
        pltpu.make_async_copy(source(trunk, y), target, recv_sem).start()

    def to_branch(source, target, send_sem, recv_sem):
        def step(i):
            other = lax.rem(branch + i, n_branch)
            send(source(other), target, send_sem, recv_sem, trunk, other)

        loop(1, n_branch, step)
        pltpu.make_async_copy(source(branch), target, recv_sem).start()

    to_served(lambda t, o: asked_ref, asked.at[me], send_sems.at[0], recv_sems.at[0])
    to_branch(
        lambda b: segment_ref.at[:, :, columns(lax.rem(b, KVH))],
        held.at[branch],
        send_sems.at[1],
        recv_sems.at[1],
    )
    send(own_ref, before, send_sems.at[2], recv_sems.at[2], trunk, after)
    send(tags_ref, before_tags, send_sems.at[3], recv_sems.at[3], trunk, after)

    def two_heads(ref, pair):
        return ref[pl.ds(2 * pair, 2)].reshape(2 * rows, DH)

    def twice(part):
        return jnp.concatenate([bias[part], bias[part]], axis=1)

    def start_part(part, pair, keys, values):
        scores = dot_nt(keys, two_heads(q, pair)) + twice(part)
        highest = jnp.max(scores, axis=0, keepdims=True)
        expo = jnp.exp2((scores - highest) * EXP2_SCALE)
        gw = dot_nt(values, two_heads(g, pair))
        total = jnp.sum(expo, axis=0, keepdims=True)
        mean = jnp.sum(expo * gw, axis=0, keepdims=True)
        return expo, gw, highest, total, mean

    def start_early(part, kv):
        def group(head):
            keys, values = kv[head, 0], kv[head, 1]
            for i in range(per_group):
                pair = head * per_group + i
                expo, gw, *rest = start_part(part + 1, pair, keys, values)
                early[part, pair] = expo
                early_gw[part, pair] = gw
                for k in range(3):
                    stats[pair, 3 * part + k : 3 * part + k + 1] = rest[k]

        loop(0, KVH, group)

    arrived(q, load_sems.at[0])
    arrived(g, load_sems.at[1])
    start_early(1, own_ref)

    arrived(asked, recv_sems.at[0])
    local = pltpu.make_async_copy(asked, wanted, local_sem)
    local.start()
    local.wait()
    arrived(held, recv_sems.at[1])

    def pick(i):
        staged[i] = held[wanted[i, 0, trunk]]

    loop(0, n_served, pick)
    to_served(
        lambda t, o: staged.at[t * KVH + o], got.at[y, trunk], send_sems.at[4], recv_sems.at[4]
    )

    arrived(before_tags, recv_sems.at[3])
    earlier_tags = jnp.where(branch > 0, before_tags[...], -1)
    bias[1] = jnp.where(jnp.broadcast_to(earlier_tags, (rows, rows)).T == squares, 0.0, NEG)
    arrived(before, recv_sems.at[2])
    start_early(0, before)

    arrived(got, recv_sems.at[4])

    def fetched(head, part):
        return got[head, :, part].reshape(trunk_len, DH)

    def all_pairs(ref, head):
        return jnp.concatenate([ref[head * per_group + i] for i in range(per_group)], axis=1)

    def all_heads(ref, head):
        return ref[pl.ds(head * 2 * per_group, 2 * per_group)].reshape(2 * per_group * rows, DH)

    def trunk_group(head):
        keys, values = fetched(head, 0), fetched(head, 1)
        for i in range(per_group):
            pair = head * per_group + i
            expo, gw, highest, total, mean = start_part(0, pair, keys, values)
            best = jnp.maximum(highest, jnp.maximum(stats[pair, 0:1], stats[pair, 3:4]))
            factors = [jnp.exp2((m - best) * EXP2_SCALE) for m in (stats[pair, 0:1], stats[pair, 3:4], highest)]
            totals = (stats[pair, 1:2], stats[pair, 4:5], total)
            means = (stats[pair, 2:3], stats[pair, 5:6], mean)
            norm = 1.0 / sum(f * t for f, t in zip(factors, totals))
            factors = [f * norm for f in factors]
            row_mean = sum(f * t for f, t in zip(factors, means))
            stats[pair, 0:1] = factors[0]
            stats[pair, 1:2] = factors[1]
            stats[pair, 2:3] = row_mean
            w = expo * factors[2]
            weights[pair] = w.astype(jnp.bfloat16)
            grads[pair] = (w * (gw - row_mean)).astype(jnp.bfloat16)
        dk = dot(all_pairs(grads, head), all_heads(q, head)) * SCALE
        dv = dot(all_pairs(weights, head), all_heads(g, head))
        for part, grad in enumerate((dk, dv)):
            dtrunk[head, :, part] = grad.reshape(n_trunk, -1, DH).astype(jnp.bfloat16)

        def give(i):
            t = lax.rem(trunk + i, n_trunk)
            send(dtrunk.at[head, t], came.at[me], send_sems.at[5], recv_sems.at[5], t, z * KVH + head)

        @pl.when(head != y)
        def _():
            give(0)

        @pl.when(head == y)
        def _():
            pltpu.make_async_copy(dtrunk.at[head, trunk], came.at[me], recv_sems.at[5]).start()

        loop(1, n_trunk, give)

    loop(0, KVH, trunk_group)

    def rest_group(head):
        key_cols = jnp.concatenate([fetched(head, 0), before[head, 0], own_ref[head, 0]], axis=0).T
        value_cols = jnp.concatenate([fetched(head, 1), before[head, 1], own_ref[head, 1]], axis=0).T
        w_parts, sg_parts = [], []
        for i in range(per_group):
            pair = head * per_group + i
            row_mean = stats[pair, 2:3]
            w_bf, sg = [], []
            for part in range(2):
                w = early[part, pair] * stats[pair, part : part + 1]
                w_bf.append(w.astype(jnp.bfloat16))
                sg.append((w * (early_gw[part, pair] - row_mean)).astype(jnp.bfloat16))
            w_bf, sg = jnp.concatenate(w_bf, axis=0), jnp.concatenate(sg, axis=0)
            w_parts.append(w_bf)
            sg_parts.append(sg)
            out = dot(value_cols, jnp.concatenate([weights[pair], w_bf], axis=0))
            dq = dot(key_cols, jnp.concatenate([grads[pair], sg], axis=0)) * SCALE
            for k in range(2):
                half = slice(k * rows, (k + 1) * rows)
                att[2 * pair + k] = out[:, half].T.astype(jnp.bfloat16)
                qg[2 * pair + k] = dq[:, half].T.astype(jnp.bfloat16)
        dk = dot(jnp.concatenate(sg_parts, axis=1), all_heads(q, head)) * SCALE
        dv = dot(jnp.concatenate(w_parts, axis=1), all_heads(g, head))
        for part, grad in enumerate((dk, dv)):
            dbefore[head, part] = grad[:rows].astype(jnp.bfloat16)
            down[head, part] = grad[rows:]
        send(dbefore.at[head], after_grad.at[head], send_sems.at[6], recv_sems.at[6], trunk, previous)

        def store(i):
            at = head * 2 * per_group + i
            pltpu.make_async_copy(att.at[at], att_hbm.at[:, columns(at)], store_sems.at[0]).start()
            pltpu.make_async_copy(qg.at[at], qg_hbm.at[:, columns(at)], store_sems.at[1]).start()

        loop(0, 2 * per_group, store)

    loop(0, HEADS_BEFORE_SUMS, rest_group)

    arrived(came, recv_sems.at[5])

    def add_up(owner):
        total = jnp.zeros(came.shape[1:], jnp.float32)
        for i in range(n_served):
            hit = jnp.where(wanted[i, 0, trunk] == owner, 1.0, 0.0)
            total = total + came[i].astype(jnp.float32) * hit
        summed[owner] = total.astype(jnp.bfloat16)

    loop(0, n_branch, add_up)
    to_branch(lambda b: summed.at[b], sums.at[branch], send_sems.at[7], recv_sems.at[7])

    loop(HEADS_BEFORE_SUMS, KVH, rest_group)

    arrived(after_grad, recv_sems.at[6])

    def finish(head):
        kv_grad_ref[head] = down[head] + after_grad[head].astype(jnp.float32)

    loop(0, KVH, finish)
    arrived(sums, recv_sems.at[7])
    for head in range(KVH):
        total = sums[head].astype(jnp.float32)
        for i in range(1, n_branch // KVH):
            total = total + sums[i * KVH + head].astype(jnp.float32)
        trunk_grad_ref[:, :, head * DH : (head + 1) * DH] = total

    others = pl.ds(0, n_served - 1)
    arrived(asked.at[others], send_sems.at[0])
    arrived(held.at[pl.ds(0, n_branch - 1)], send_sems.at[1])
    arrived(own_ref, send_sems.at[2])
    arrived(tags_ref, send_sems.at[3])
    arrived(staged.at[others], send_sems.at[4])
    arrived(came.at[others], send_sems.at[5])
    arrived(dbefore, send_sems.at[6])
    arrived(sums.at[pl.ds(0, n_branch - 1)], send_sems.at[7])
    arrived(att, store_sems.at[0])
    arrived(qg, store_sems.at[1])


def fused(n_trunk, n_branch, queries, out_grad, own, segment, asked, tags, reach):
    rows, width = queries.shape
    n_served = n_trunk * KVH
    heads = width // DH
    piece = (2, segment.shape[1], DH)
    trunk_len = n_trunk * segment.shape[1]
    vmem = pl.BlockSpec(memory_space=pltpu.VMEM)
    anywhere = pl.BlockSpec(memory_space=pl.ANY)
    bf16, f32 = jnp.bfloat16, jnp.float32
    return pl.pallas_call(
        functools.partial(kernel, n_trunk, n_branch),
        in_specs=[anywhere] * 2 + [vmem] * 5,
        out_specs=[anywhere] * 2 + [vmem] * 2,
        out_shape=[
            jax.ShapeDtypeStruct(queries.shape, bf16),
            jax.ShapeDtypeStruct(queries.shape, bf16),
            jax.ShapeDtypeStruct(own.shape, f32),
            jax.ShapeDtypeStruct(segment.shape, f32),
        ],
        scratch_shapes=[
            pltpu.VMEM((heads, rows, DH), bf16),
            pltpu.VMEM((heads, rows, DH), bf16),
            pltpu.VMEM((n_branch, *piece), bf16),
            pltpu.VMEM((n_served, *asked.shape), jnp.int32),
            pltpu.SMEM((n_served, *asked.shape), jnp.int32),
            pltpu.VMEM((n_served, *piece), bf16),
            pltpu.VMEM((KVH, n_trunk, *piece), bf16),
            pltpu.VMEM(own.shape, bf16),
            pltpu.VMEM(tags.shape, jnp.int32),
            pltpu.VMEM((3, rows, rows), f32),
            pltpu.VMEM((2, heads // 2, rows, 2 * rows), f32),
            pltpu.VMEM((2, heads // 2, rows, 2 * rows), f32),
            pltpu.VMEM((heads // 2, 8, 2 * rows), f32),
            pltpu.VMEM((heads // 2, trunk_len, 2 * rows), bf16),
            pltpu.VMEM((heads // 2, trunk_len, 2 * rows), bf16),
            pltpu.VMEM((heads, rows, DH), bf16),
            pltpu.VMEM((heads, rows, DH), bf16),
            pltpu.VMEM((KVH, n_trunk, *piece), bf16),
            pltpu.VMEM(own.shape, bf16),
            pltpu.VMEM(own.shape, f32),
            pltpu.VMEM((n_served, *piece), bf16),
            pltpu.VMEM((n_branch, *piece), bf16),
            pltpu.VMEM((n_branch, *piece), bf16),
            pltpu.VMEM(own.shape, bf16),
            pltpu.SemaphoreType.DMA((2,)),
            pltpu.SemaphoreType.DMA((2,)),
            pltpu.SemaphoreType.DMA,
            pltpu.SemaphoreType.DMA((8,)),
            pltpu.SemaphoreType.DMA((8,)),
        ],
        compiler_params=pltpu.CompilerParams(collective_id=0, has_side_effects=True),
        name="tree_attention",
    )(queries, out_grad, own, segment, asked, tags, reach)


def on_device(queries, keys_values, out_grad, trunk_kv, branch_of, branch_reach, ancestors):
    n_trunk, n_branch = lax.axis_size("trunk"), lax.axis_size("branch")
    rows, _, width = keys_values.shape[1:]
    own = keys_values[0].reshape(rows, 2, KVH, DH).transpose(2, 1, 0, 3)
    asked = jnp.pad(ancestors[0], ((0, 0), (0, DH - n_trunk)))
    attended, query_grad, kv_grad, trunk_grad = fused(
        n_trunk, n_branch, queries[0], out_grad[0], own, trunk_kv[0, 0], asked, branch_of, branch_reach
    )
    kv_grad = kv_grad.transpose(2, 1, 0, 3).reshape(rows, 2, width)
    return (attended[None], query_grad[None], kv_grad[None], trunk_grad[None, None])


def solution(mesh):
    return jax.shard_map(
        on_device,
        mesh=mesh,
        in_specs=(
            P("trunk", "branch", None),
            P("trunk", "branch", None, None),
            P("trunk", "branch", None),
            P("trunk", "branch", None, None, None),
            P("trunk", "branch"),
            P("trunk", None),
            P("trunk", "branch", None),
        ),
        out_specs=(
            P("trunk", "branch", None),
            P("trunk", "branch", None),
            P("trunk", "branch", None, None),
            P("trunk", "branch", None, None, None),
        ),
        check_vma=False,
    )
```

```python
import functools
import math

import jax
import jax.numpy as jnp
from jax import lax
from jax.experimental import pallas as pl
from jax.experimental.pallas import tpu as pltpu
from jax.sharding import PartitionSpec as P

KVH = 4
DH = 128
NEG = -1e30
SCALE = 1.0 / math.sqrt(DH)
EXP2_SCALE = SCALE * math.log2(math.e)
MESH = pl.DeviceIdType.MESH
NT = (((1,), (1,)), ((), ()))
HEADS_BEFORE_SUMS = 2


def dot(a, b):
    return jnp.dot(a, b, preferred_element_type=jnp.float32)


def dot_nt(a, b):
    return lax.dot_general(a, b, NT, preferred_element_type=jnp.float32)


def signal(semaphore, trunk, branch):
    pl.semaphore_signal(semaphore, inc=1, device_id=(trunk, branch), device_id_type=MESH)


def send(source, target, send_sem, recv_sem, trunk, branch):
    pltpu.make_async_remote_copy(
        src_ref=source,
        dst_ref=target,
        send_sem=send_sem,
        recv_sem=recv_sem,
        device_id=(trunk, branch),
        device_id_type=MESH,
    ).start()


def arrived(ref, sem):
    pltpu.make_async_copy(ref, ref, sem).wait()


def loop(first, last, body):
    def step(i, carry):
        body(i)
        return carry

    lax.fori_loop(first, last, step, 0)


def far_first(i, n):
    return lax.rem(n // 2 + (i + 1) // 2 * (2 * lax.rem(i, 2) - 1) * -1 + n, n)


def columns(head):
    return pl.ds(pl.multiple_of(head * DH, DH), DH)


def split_up(raw, kv):
    for part in range(2):
        both = raw[:, part, :]
        for head in range(KVH):
            kv[head, part] = both[:, head * DH : (head + 1) * DH]


def kernel(
    n_trunk, n_branch,
    q_hbm, g_hbm, own_hbm, segment_hbm, asked_hbm, tags_hbm, reach_hbm,
    att_out, qg_out, kv_out, trunk_out,
    q, g, own_raw, segment_ref, asked_ref, tags_ref, reach_ref, kv_grad_ref, trunk_grad_ref, held, asked, wanted, staged, got, before_raw, own_ref, before, before_tags, bias, early, early_gw, stats,
    weights, grads, att, qg, dtrunk, dbefore, down, came, summed, sums, after_grad,
    load_sems, store_sems, local_sem, send_sems, recv_sems,
):
    trunk, branch = lax.axis_index("trunk"), lax.axis_index("branch")
    z, y = branch // KVH, lax.rem(branch, KVH)
    me = trunk * KVH + y
    n_served = n_trunk * KVH
    heads = q.shape[0]
    pairs = heads // 2
    per_group = pairs // KVH
    rows = q.shape[1]
    trunk_len = n_trunk * segment_ref.shape[1]
    after = lax.rem(branch + 1, n_branch)
    previous = lax.rem(branch + n_branch - 1, n_branch)

    def in_branch(i):
        dz, dy = far_first(i // KVH, n_branch // KVH), far_first(lax.rem(i, KVH), KVH)
        return lax.rem(z + dz, n_branch // KVH) * KVH + lax.rem(y + dy, KVH)

    def in_served(i):
        dt, dy = far_first(i // KVH, n_trunk), far_first(lax.rem(i, KVH), KVH)
        return lax.rem(trunk + dt, n_trunk), lax.rem(y + dy, KVH)

    barrier = pltpu.get_barrier_semaphore()
    loop(0, n_branch - 1, lambda i: signal(barrier, trunk, in_branch(i)))

    def greet(i):
        t, other = in_served(i)
        signal(barrier, t, z * KVH + other)

    loop(0, (n_trunk - 1) * KVH, greet)

    def load(i):
        pltpu.make_async_copy(q_hbm.at[:, columns(i)], q.at[i], load_sems.at[0]).start()
        pltpu.make_async_copy(g_hbm.at[:, columns(i)], g.at[i], load_sems.at[1]).start()

    inputs = [
        pltpu.make_async_copy(source, target, load_sems.at[2 + i])
        for i, (source, target) in enumerate(
            (
                (tags_hbm, tags_ref),
                (reach_hbm, reach_ref),
                (asked_hbm, asked_ref),
                (segment_hbm, segment_ref),
                (own_hbm, own_raw),
            )
        )
    ]
    for copy in inputs:
        copy.start()
    loop(0, heads, load)
    for copy in inputs:
        copy.wait()

    split_up(own_raw, own_ref)
    squares = jnp.broadcast_to(tags_ref[...], (rows, rows))
    position = lax.broadcasted_iota(jnp.int32, (rows, rows), 0)
    query = lax.broadcasted_iota(jnp.int32, (rows, rows), 1)
    bias[2] = jnp.where((squares.T == squares) & (position <= query), 0.0, NEG)
    branches = reach_ref.shape[1]
    reach_column = jnp.broadcast_to(reach_ref[...].astype(jnp.float32), (branches, branches)).T
    branch_index = lax.broadcasted_iota(jnp.int32, (branches, rows), 0)
    reach = jnp.sum(
        jnp.where(branch_index == tags_ref[...], reach_column[:, :1], 0.0), axis=0, keepdims=True
    )
    depth = lax.broadcasted_iota(jnp.int32, (trunk_len, rows), 0) // segment_ref.shape[1]
    bias[0] = jnp.where(depth.astype(jnp.float32) < reach, 0.0, NEG)

    pl.semaphore_wait(barrier, n_branch - 1 + (n_trunk - 1) * KVH)

    def to_served(source, target, send_sem, recv_sem):
        def step(i):
            t, other = in_served(i)
            send(source(t, other), target, send_sem, recv_sem, t, z * KVH + other)

        loop(0, n_served - 1, step)
        pltpu.make_async_copy(source(trunk, y), target, recv_sem).start()

    def to_branch(source, target, send_sem, recv_sem):
        def step(i):
            other = in_branch(i)
            send(source(other), target, send_sem, recv_sem, trunk, other)

        loop(0, n_branch - 1, step)
        pltpu.make_async_copy(source(branch), target, recv_sem).start()

    to_served(lambda t, o: asked_ref, asked.at[me], send_sems.at[0], recv_sems.at[0])
    to_branch(
        lambda b: segment_ref.at[:, :, columns(lax.rem(b, KVH))],
        held.at[branch],
        send_sems.at[1],
        recv_sems.at[1],
    )
    send(own_raw, before_raw, send_sems.at[2], recv_sems.at[2], trunk, after)
    send(tags_ref, before_tags, send_sems.at[3], recv_sems.at[3], trunk, after)

    def two_heads(ref, pair):
        return ref[pl.ds(2 * pair, 2)].reshape(2 * rows, DH)

    def twice(part):
        return jnp.concatenate([bias[part], bias[part]], axis=1)

    def start_part(part, pair, keys, values):
        scores = dot_nt(keys, two_heads(q, pair)) + twice(part)
        highest = jnp.max(scores, axis=0, keepdims=True)
        expo = jnp.exp2((scores - highest) * EXP2_SCALE)
        gw = dot_nt(values, two_heads(g, pair))
        total = jnp.sum(expo, axis=0, keepdims=True)
        mean = jnp.sum(expo * gw, axis=0, keepdims=True)
        return expo, gw, highest, total, mean

    def start_early(part, kv):
        def group(head):
            keys, values = kv[head, 0], kv[head, 1]
            for i in range(per_group):
                pair = head * per_group + i
                expo, gw, *rest = start_part(part + 1, pair, keys, values)
                early[part, pair] = expo
                early_gw[part, pair] = gw
                for k in range(3):
                    stats[pair, 3 * part + k : 3 * part + k + 1] = rest[k]

        loop(0, KVH, group)

    arrived(q, load_sems.at[0])
    arrived(g, load_sems.at[1])
    start_early(1, own_ref)

    arrived(asked, recv_sems.at[0])
    local = pltpu.make_async_copy(asked, wanted, local_sem)
    local.start()
    local.wait()
    arrived(held, recv_sems.at[1])

    def pick(i):
        staged[i] = held[wanted[i, 0, trunk]]

    loop(0, n_served, pick)
    to_served(
        lambda t, o: staged.at[t * KVH + o], got.at[y, trunk], send_sems.at[4], recv_sems.at[4]
    )

    arrived(before_tags, recv_sems.at[3])
    earlier_tags = jnp.where(branch > 0, before_tags[...], -1)
    bias[1] = jnp.where(jnp.broadcast_to(earlier_tags, (rows, rows)).T == squares, 0.0, NEG)
    arrived(before_raw, recv_sems.at[2])
    split_up(before_raw, before)
    start_early(0, before)

    arrived(got, recv_sems.at[4])

    def fetched(head, part):
        return got[head, :, part].reshape(trunk_len, DH)

    def all_heads(ref, head):
        return ref[pl.ds(head * 2 * per_group, 2 * per_group)].reshape(2 * per_group * rows, DH)

    def trunk_group(turn):
        head = lax.rem(y + far_first(turn, KVH), KVH)
        keys, values = fetched(head, 0), fetched(head, 1)
        known = [stats[head * per_group + i] for i in range(per_group)]
        merged, w_parts, sg_parts = [], [], []
        for i in range(per_group):
            pair = head * per_group + i
            expo, gw, highest, total, mean = start_part(0, pair, keys, values)
            peaks, totals, means = [
                [known[i][k : k + 1], known[i][k + 3 : k + 4], last]
                for k, last in enumerate((highest, total, mean))
            ]
            best = jnp.maximum(peaks[2], jnp.maximum(peaks[0], peaks[1]))
            factors = [jnp.exp2((m - best) * EXP2_SCALE) for m in peaks]
            norm = 1.0 / sum(f * t for f, t in zip(factors, totals))
            factors = [f * norm for f in factors]
            row_mean = sum(f * t for f, t in zip(factors, means))
            merged.append((factors[0], factors[1], row_mean))
            w = expo * factors[2]
            w_parts.append(w.astype(jnp.bfloat16))
            sg_parts.append((w * (gw - row_mean)).astype(jnp.bfloat16))
        dv = dot(jnp.concatenate(w_parts, axis=1), all_heads(g, head))
        dk = dot(jnp.concatenate(sg_parts, axis=1), all_heads(q, head)) * SCALE
        for part, grad in enumerate((dk, dv)):
            dtrunk[head, :, part] = grad.reshape(n_trunk, -1, DH).astype(jnp.bfloat16)

        def give(i):
            t = lax.rem(trunk + far_first(i, n_trunk), n_trunk)
            send(dtrunk.at[head, t], came.at[me], send_sems.at[5], recv_sems.at[5], t, z * KVH + head)

        loop(0, n_trunk - 1, give)

        @pl.when(head != y)
        def _():
            give(n_trunk - 1)

        @pl.when(head == y)
        def _():
            pltpu.make_async_copy(dtrunk.at[head, trunk], came.at[me], recv_sems.at[5]).start()

        for i in range(per_group):
            pair = head * per_group + i
            for k in range(3):
                stats[pair, k : k + 1] = merged[i][k]
            weights[pair] = w_parts[i]
            grads[pair] = sg_parts[i]

    loop(0, KVH, trunk_group)

    def rest_group(head):
        key_cols = jnp.concatenate([fetched(head, 0), before[head, 0], own_ref[head, 0]], axis=0).T
        value_cols = jnp.concatenate([fetched(head, 1), before[head, 1], own_ref[head, 1]], axis=0).T
        w_parts, sg_parts = [], []
        for i in range(per_group):
            pair = head * per_group + i
            row_mean = stats[pair, 2:3]
            w_bf, sg = [], []
            for part in range(2):
                w = early[part, pair] * stats[pair, part : part + 1]
                w_bf.append(w.astype(jnp.bfloat16))
                sg.append((w * (early_gw[part, pair] - row_mean)).astype(jnp.bfloat16))
            w_bf, sg = jnp.concatenate(w_bf, axis=0), jnp.concatenate(sg, axis=0)
            w_parts.append(w_bf)
            sg_parts.append(sg)
            out = dot(value_cols, jnp.concatenate([weights[pair], w_bf], axis=0))
            dq = dot(key_cols, jnp.concatenate([grads[pair], sg], axis=0)) * SCALE
            for k in range(2):
                half = slice(k * rows, (k + 1) * rows)
                att[2 * pair + k] = out[:, half].T.astype(jnp.bfloat16)
                qg[2 * pair + k] = dq[:, half].T.astype(jnp.bfloat16)
        dk = dot(jnp.concatenate(sg_parts, axis=1), all_heads(q, head)) * SCALE
        dv = dot(jnp.concatenate(w_parts, axis=1), all_heads(g, head))
        for part, grad in enumerate((dk, dv)):
            dbefore[head, part] = grad[:rows].astype(jnp.bfloat16)
            down[head, part] = grad[rows:]
        send(dbefore.at[head], after_grad.at[head], send_sems.at[6], recv_sems.at[6], trunk, previous)

        def store(i):
            at = head * 2 * per_group + i
            pltpu.make_async_copy(att.at[at], att_out.at[:, columns(at)], store_sems.at[0]).start()
            pltpu.make_async_copy(qg.at[at], qg_out.at[:, columns(at)], store_sems.at[1]).start()

        loop(0, 2 * per_group, store)

    loop(0, HEADS_BEFORE_SUMS, rest_group)

    arrived(came, recv_sems.at[5])

    def add_up(owner):
        total = jnp.zeros(came.shape[1:], jnp.float32)
        for i in range(n_served):
            hit = jnp.where(wanted[i, 0, trunk] == owner, 1.0, 0.0)
            total = total + came[i].astype(jnp.float32) * hit
        summed[owner] = total.astype(jnp.bfloat16)

    loop(0, n_branch, add_up)
    to_branch(lambda b: summed.at[b], sums.at[branch], send_sems.at[7], recv_sems.at[7])

    loop(HEADS_BEFORE_SUMS, KVH, rest_group)

    arrived(after_grad, recv_sems.at[6])

    def finish(head):
        kv_grad_ref[head] = down[head] + after_grad[head].astype(jnp.float32)

    loop(0, KVH, finish)
    kv_copy = pltpu.make_async_copy(kv_grad_ref, kv_out, store_sems.at[2])
    kv_copy.start()
    arrived(sums, recv_sems.at[7])
    for head in range(KVH):
        total = sums[head].astype(jnp.float32)
        for i in range(1, n_branch // KVH):
            total = total + sums[i * KVH + head].astype(jnp.float32)
        trunk_grad_ref[:, :, head * DH : (head + 1) * DH] = total

    trunk_copy = pltpu.make_async_copy(trunk_grad_ref, trunk_out, store_sems.at[3])
    trunk_copy.start()
    others = pl.ds(0, n_served - 1)
    arrived(asked.at[others], send_sems.at[0])
    arrived(held.at[pl.ds(0, n_branch - 1)], send_sems.at[1])
    arrived(own_raw, send_sems.at[2])
    arrived(tags_ref, send_sems.at[3])
    arrived(staged.at[others], send_sems.at[4])
    arrived(came.at[others], send_sems.at[5])
    arrived(dbefore, send_sems.at[6])
    arrived(sums.at[pl.ds(0, n_branch - 1)], send_sems.at[7])
    arrived(att, store_sems.at[0])
    arrived(qg, store_sems.at[1])
    kv_copy.wait()
    trunk_copy.wait()


def fused(n_trunk, n_branch, queries, out_grad, own, segment, asked, tags, reach):
    rows, width = queries.shape
    n_served = n_trunk * KVH
    heads = width // DH
    piece = (2, segment.shape[1], DH)
    trunk_len = n_trunk * segment.shape[1]
    by_head = (KVH, 2, rows, DH)
    anywhere = pl.BlockSpec(memory_space=pl.ANY)
    bf16, f32 = jnp.bfloat16, jnp.float32
    return pl.pallas_call(
        functools.partial(kernel, n_trunk, n_branch),
        in_specs=[pl.BlockSpec(memory_space=pltpu.HBM)] * 7,
        out_specs=[anywhere] * 4,
        out_shape=[
            jax.ShapeDtypeStruct(queries.shape, bf16),
            jax.ShapeDtypeStruct(queries.shape, bf16),
            jax.ShapeDtypeStruct(by_head, f32),
            jax.ShapeDtypeStruct(segment.shape, f32),
        ],
        scratch_shapes=[
            pltpu.VMEM((heads, rows, DH), bf16),
            pltpu.VMEM((heads, rows, DH), bf16),
            *[pltpu.VMEM(a.shape, a.dtype) for a in (own, segment, asked, tags, reach)],
            pltpu.VMEM(by_head, f32),
            pltpu.VMEM(segment.shape, f32),
            pltpu.VMEM((n_branch, *piece), bf16),
            pltpu.VMEM((n_served, *asked.shape), jnp.int32),
            pltpu.SMEM((n_served, *asked.shape), jnp.int32),
            pltpu.VMEM((n_served, *piece), bf16),
            pltpu.VMEM((KVH, n_trunk, *piece), bf16),
            pltpu.VMEM(own.shape, bf16),
            pltpu.VMEM(by_head, bf16),
            pltpu.VMEM(by_head, bf16),
            pltpu.VMEM(tags.shape, jnp.int32),
            pltpu.VMEM((3, rows, rows), f32),
            pltpu.VMEM((2, heads // 2, rows, 2 * rows), f32),
            pltpu.VMEM((2, heads // 2, rows, 2 * rows), f32),
            pltpu.VMEM((heads // 2, 8, 2 * rows), f32),
            pltpu.VMEM((heads // 2, trunk_len, 2 * rows), bf16),
            pltpu.VMEM((heads // 2, trunk_len, 2 * rows), bf16),
            pltpu.VMEM((heads, rows, DH), bf16),
            pltpu.VMEM((heads, rows, DH), bf16),
            pltpu.VMEM((KVH, n_trunk, *piece), bf16),
            pltpu.VMEM(by_head, bf16),
            pltpu.VMEM(by_head, f32),
            pltpu.VMEM((n_served, *piece), bf16),
            pltpu.VMEM((n_branch, *piece), bf16),
            pltpu.VMEM((n_branch, *piece), bf16),
            pltpu.VMEM(by_head, bf16),
            pltpu.SemaphoreType.DMA((7,)),
            pltpu.SemaphoreType.DMA((4,)),
            pltpu.SemaphoreType.DMA,
            pltpu.SemaphoreType.DMA((8,)),
            pltpu.SemaphoreType.DMA((8,)),
        ],
        compiler_params=pltpu.CompilerParams(
            collective_id=0, has_side_effects=True, vmem_limit_bytes=40 << 20
        ),
        name="tree_attention",
    )(queries, out_grad, own, segment, asked, tags, reach)


def assemble_kernel(
    att_in, qg_in, kv_in, trunk_in, att_out, qg_out, kv_out, trunk_out, kv, kv_rows, sems
):
    first = pltpu.make_async_copy(kv_in, kv, sems.at[0])
    direct = [
        pltpu.make_async_copy(att_in, att_out, sems.at[1]),
        pltpu.make_async_copy(qg_in, qg_out, sems.at[2]),
        pltpu.make_async_copy(trunk_in, trunk_out, sems.at[3]),
    ]
    last = pltpu.make_async_copy(kv_rows, kv_out, sems.at[4])
    for copy in [first, *direct]:
        copy.start()
    first.wait()
    for part in range(2):
        for head in range(KVH):
            kv_rows[:, part, head * DH : (head + 1) * DH] = kv[head, part]
    last.start()
    for copy in [*direct, last]:
        copy.wait()


def assemble(att, qg, kv_grad, trunk_grad):
    anywhere = pl.BlockSpec(memory_space=pl.ANY)
    heads, parts, rows, width = kv_grad.shape
    kv_rows = jax.ShapeDtypeStruct((rows, parts, heads * width), kv_grad.dtype)
    return pl.pallas_call(
        assemble_kernel,
        in_specs=[anywhere] * 4,
        out_specs=[anywhere] * 4,
        out_shape=[jax.ShapeDtypeStruct(a.shape, a.dtype) for a in (att, qg, kv_rows, trunk_grad)],
        scratch_shapes=[
            pltpu.VMEM(kv_grad.shape, kv_grad.dtype),
            pltpu.VMEM(kv_rows.shape, kv_rows.dtype),
            pltpu.SemaphoreType.DMA((5,)),
        ],
        compiler_params=pltpu.CompilerParams(vmem_limit_bytes=8 << 20),
        name="assemble",
    )(att, qg, kv_grad, trunk_grad)


def on_device(queries, keys_values, out_grad, trunk_kv, branch_of, branch_reach, ancestors):
    n_trunk, n_branch = lax.axis_size("trunk"), lax.axis_size("branch")
    arrays = (queries[0], out_grad[0], keys_values[0], trunk_kv[0, 0], ancestors[0], branch_of, branch_reach)
    arrays = [pltpu.with_memory_space_constraint(a, pltpu.HBM) for a in arrays]
    results = fused(n_trunk, n_branch, *arrays)
    attended, query_grad, kv_grad, trunk_grad = assemble(*results)
    return (attended[None], query_grad[None], kv_grad[None], trunk_grad[None, None])


def solution(mesh):
    return jax.shard_map(
        on_device,
        mesh=mesh,
        in_specs=(
            P("trunk", "branch", None),
            P("trunk", "branch", None, None),
            P("trunk", "branch", None),
            P("trunk", "branch", None, None, None),
            P("trunk", "branch"),
            P("trunk", None),
            P("trunk", "branch", None),
        ),
        out_specs=(
            P("trunk", "branch", None),
            P("trunk", "branch", None),
            P("trunk", "branch", None, None),
            P("trunk", "branch", None, None, None),
        ),
        check_vma=False,
    )
```

```python
import functools
import math

import jax
import jax.numpy as jnp
from jax import lax
from jax.experimental import pallas as pl
from jax.experimental.pallas import tpu as pltpu
from jax.sharding import PartitionSpec as P

KVH = 4
DH = 128
NEG = -1e30
SCALE = 1.0 / math.sqrt(DH)
EXP2_SCALE = SCALE * math.log2(math.e)
MESH = pl.DeviceIdType.MESH
NT = (((1,), (1,)), ((), ()))
HEADS_BEFORE_SUMS = 2


def dot(a, b):
    return jnp.dot(a, b, preferred_element_type=jnp.float32)


def dot_nt(a, b):
    return lax.dot_general(a, b, NT, preferred_element_type=jnp.float32)


def signal(semaphore, trunk, branch):
    pl.semaphore_signal(semaphore, inc=1, device_id=(trunk, branch), device_id_type=MESH)


def send(source, target, send_sem, recv_sem, trunk, branch):
    pltpu.make_async_remote_copy(
        src_ref=source,
        dst_ref=target,
        send_sem=send_sem,
        recv_sem=recv_sem,
        device_id=(trunk, branch),
        device_id_type=MESH,
    ).start()


def arrived(ref, sem):
    pltpu.make_async_copy(ref, ref, sem).wait()


def loop(first, last, body):
    def step(i, carry):
        body(i)
        return carry

    lax.fori_loop(first, last, step, 0)


def far_first(n):
    return [(n // 2 + (i + 1) // 2 * (-1 if i % 2 else 1)) % n for i in range(n)]


def columns(head):
    return pl.ds(pl.multiple_of(head * DH, DH), DH)


def split_up(raw, kv):
    for part in range(2):
        both = raw[:, part, :]
        for head in range(KVH):
            kv[head, part] = both[:, head * DH : (head + 1) * DH]


def kernel(
    n_trunk, n_branch,
    q_hbm, g_hbm, own_hbm, segment_hbm, asked_hbm, tags_hbm, reach_hbm,
    att_out, qg_out, kv_out, trunk_out,
    q, g, own_raw, segment_ref, asked_ref, tags_ref, reach_ref, kv_grad_ref, trunk_grad_ref, held, asked, wanted, staged, got, before_raw, own_ref, before, before_tags, bias, early, early_gw, stats,
    weights, grads, att, qg, dtrunk, dbefore, down, came, hits, summed, sums, after_grad,
    load_sems, store_sems, local_sem, send_sems, recv_sems,
):
    trunk, branch = lax.axis_index("trunk"), lax.axis_index("branch")
    z, y = branch // KVH, lax.rem(branch, KVH)
    me = trunk * KVH + y
    n_served = n_trunk * KVH
    heads = q.shape[0]
    pairs = heads // 2
    per_group = pairs // KVH
    rows = q.shape[1]
    trunk_len = n_trunk * segment_ref.shape[1]
    after = lax.rem(branch + 1, n_branch)
    previous = lax.rem(branch + n_branch - 1, n_branch)

    ys = [lax.rem(y + d, KVH) for d in far_first(KVH)]
    zs = [lax.rem(z + d, n_branch // KVH) for d in far_first(n_branch // KVH)]
    ts = [lax.rem(trunk + d, n_trunk) for d in far_first(n_trunk)]
    in_branch = [at * KVH + other for at in zs for other in ys][:-1]
    in_served = [(t, other) for t in ts for other in ys][:-1]

    inputs = [
        pltpu.make_async_copy(source, target, load_sems.at[2 + i])
        for i, (source, target) in enumerate(
            (
                (asked_hbm, asked_ref),
                (segment_hbm, segment_ref),
                (own_hbm, own_raw),
                (tags_hbm, tags_ref),
                (reach_hbm, reach_ref),
            )
        )
    ]
    for copy in inputs:
        copy.start()
    barrier = pltpu.get_barrier_semaphore()
    for other in in_branch:
        signal(barrier, trunk, other)
    for t, other in in_served[: (n_trunk - 1) * KVH]:
        signal(barrier, t, z * KVH + other)
    for copy in inputs:
        copy.wait()
    pl.semaphore_wait(barrier, n_branch - 1 + (n_trunk - 1) * KVH)

    def to_served(source, target, send_sem, recv_sem):
        for t, other in in_served:
            send(source(t, other), target, send_sem, recv_sem, t, z * KVH + other)
        pltpu.make_async_copy(source(trunk, y), target, recv_sem).start()

    def to_branch(source, target, send_sem, recv_sem):
        for other in in_branch:
            send(source(other), target, send_sem, recv_sem, trunk, other)
        pltpu.make_async_copy(source(branch), target, recv_sem).start()

    to_served(lambda t, o: asked_ref, asked.at[me], send_sems.at[0], recv_sems.at[0])
    to_branch(
        lambda b: segment_ref.at[:, :, columns(lax.rem(b, KVH))],
        held.at[branch],
        send_sems.at[1],
        recv_sems.at[1],
    )
    send(own_raw, before_raw, send_sems.at[2], recv_sems.at[2], trunk, after)
    send(tags_ref, before_tags, send_sems.at[3], recv_sems.at[3], trunk, after)

    def load(i):
        pltpu.make_async_copy(q_hbm.at[:, columns(i)], q.at[i], load_sems.at[0]).start()
        pltpu.make_async_copy(g_hbm.at[:, columns(i)], g.at[i], load_sems.at[1]).start()

    loop(0, heads, load)

    split_up(own_raw, own_ref)
    squares = jnp.broadcast_to(tags_ref[...], (rows, rows))
    position = lax.broadcasted_iota(jnp.int32, (rows, rows), 0)
    query = lax.broadcasted_iota(jnp.int32, (rows, rows), 1)
    bias[2] = jnp.where((squares.T == squares) & (position <= query), 0.0, NEG)
    branches = reach_ref.shape[1]
    reach_column = jnp.broadcast_to(reach_ref[...].astype(jnp.float32), (branches, branches)).T
    branch_index = lax.broadcasted_iota(jnp.int32, (branches, rows), 0)
    reach = jnp.sum(
        jnp.where(branch_index == tags_ref[...], reach_column[:, :1], 0.0), axis=0, keepdims=True
    )
    depth = lax.broadcasted_iota(jnp.int32, (trunk_len, rows), 0) // segment_ref.shape[1]
    bias[0] = jnp.where(depth.astype(jnp.float32) < reach, 0.0, NEG)

    def two_heads(ref, pair):
        return ref[pl.ds(2 * pair, 2)].reshape(2 * rows, DH)

    def twice(part):
        return jnp.concatenate([bias[part], bias[part]], axis=1)

    def start_part(part, pair, keys, values):
        scores = dot_nt(keys, two_heads(q, pair)) + twice(part)
        highest = jnp.max(scores, axis=0, keepdims=True)
        expo = jnp.exp2((scores - highest) * EXP2_SCALE)
        gw = dot_nt(values, two_heads(g, pair))
        total = jnp.sum(expo, axis=0, keepdims=True)
        mean = jnp.sum(expo * gw, axis=0, keepdims=True)
        return expo, gw, highest, total, mean

    def start_early(part, kv):
        def group(head):
            keys, values = kv[head, 0], kv[head, 1]
            for i in range(per_group):
                pair = head * per_group + i
                expo, gw, *rest = start_part(part + 1, pair, keys, values)
                early[part, pair] = expo
                early_gw[part, pair] = gw
                for k in range(3):
                    stats[pair, 3 * part + k : 3 * part + k + 1] = rest[k]

        loop(0, KVH, group)

    arrived(q, load_sems.at[0])
    arrived(g, load_sems.at[1])
    start_early(1, own_ref)

    arrived(asked, recv_sems.at[0])
    local = pltpu.make_async_copy(asked, wanted, local_sem)
    local.start()
    local.wait()

    piece_rows = 2 * segment_ref.shape[1]
    lane = lax.broadcasted_iota(jnp.int32, (piece_rows, DH), 1)
    line = lax.broadcasted_iota(jnp.int32, (piece_rows, DH), 0)
    diagonal = jnp.where(lax.rem(lane, piece_rows) == line, 1.0, 0.0)
    per_tile = DH // piece_rows
    sources = []
    for tile in range(n_served // per_tile):
        source = jnp.full((piece_rows, DH), wanted[tile * per_tile, 0, trunk], jnp.int32)
        for i in range(1, per_tile):
            source = jnp.where(lane >= i * piece_rows, wanted[tile * per_tile + i, 0, trunk], source)
        sources.append(source)

    def mark(owner):
        for tile, source in enumerate(sources):
            hits[owner, :, tile * DH : (tile + 1) * DH] = jnp.where(source == owner, diagonal, 0.0).astype(
                jnp.bfloat16
            )

    loop(0, n_branch, mark)
    arrived(held, recv_sems.at[1])

    def pick(i):
        staged[i] = held[wanted[i, 0, trunk]]

    loop(0, n_served, pick)
    to_served(
        lambda t, o: staged.at[t * KVH + o], got.at[y, trunk], send_sems.at[4], recv_sems.at[4]
    )

    arrived(before_tags, recv_sems.at[3])
    earlier_tags = jnp.where(branch > 0, before_tags[...], -1)
    bias[1] = jnp.where(jnp.broadcast_to(earlier_tags, (rows, rows)).T == squares, 0.0, NEG)
    arrived(before_raw, recv_sems.at[2])
    split_up(before_raw, before)
    start_early(0, before)

    arrived(got, recv_sems.at[4])

    def fetched(head, part):
        return got[head, :, part].reshape(trunk_len, DH)

    def all_heads(ref, head):
        return ref[pl.ds(head * 2 * per_group, 2 * per_group)].reshape(2 * per_group * rows, DH)

    def trunk_group(turn):
        head = lax.rem(y + KVH // 2 + lax.div(turn + 1, 2) * (1 - 2 * lax.rem(turn, 2)) + KVH, KVH)
        keys, values = fetched(head, 0), fetched(head, 1)
        known = [stats[head * per_group + i] for i in range(per_group)]
        merged, w_parts, sg_parts = [], [], []
        for i in range(per_group):
            pair = head * per_group + i
            expo, gw, highest, total, mean = start_part(0, pair, keys, values)
            peaks, totals, means = [
                [known[i][k : k + 1], known[i][k + 3 : k + 4], last]
                for k, last in enumerate((highest, total, mean))
            ]
            best = jnp.maximum(peaks[2], jnp.maximum(peaks[0], peaks[1]))
            factors = [jnp.exp2((m - best) * EXP2_SCALE) for m in peaks]
            norm = 1.0 / sum(f * t for f, t in zip(factors, totals))
            factors = [f * norm for f in factors]
            row_mean = sum(f * t for f, t in zip(factors, means))
            merged.append((factors[0], factors[1], row_mean))
            w = expo * factors[2]
            w_parts.append(w.astype(jnp.bfloat16))
            sg_parts.append((w * (gw - row_mean)).astype(jnp.bfloat16))
        dv = dot(jnp.concatenate(w_parts, axis=1), all_heads(g, head))
        dk = dot(jnp.concatenate(sg_parts, axis=1), all_heads(q, head)) * SCALE
        for part, grad in enumerate((dk, dv)):
            dtrunk[head, :, part] = grad.reshape(n_trunk, -1, DH).astype(jnp.bfloat16)

        def give(t):
            send(dtrunk.at[head, t], came.at[me], send_sems.at[5], recv_sems.at[5], t, z * KVH + head)

        for t in ts[:-1]:
            give(t)

        @pl.when(head != y)
        def _():
            give(trunk)

        @pl.when(head == y)
        def _():
            pltpu.make_async_copy(dtrunk.at[head, trunk], came.at[me], recv_sems.at[5]).start()

        for i in range(per_group):
            pair = head * per_group + i
            for k in range(3):
                stats[pair, k : k + 1] = merged[i][k]
            weights[pair] = w_parts[i]
            grads[pair] = sg_parts[i]

    loop(0, KVH, trunk_group)

    def rest_group(head):
        key_cols = jnp.concatenate([fetched(head, 0), before[head, 0], own_ref[head, 0]], axis=0).T
        value_cols = jnp.concatenate([fetched(head, 1), before[head, 1], own_ref[head, 1]], axis=0).T
        w_parts, sg_parts = [], []
        for i in range(per_group):
            pair = head * per_group + i
            row_mean = stats[pair, 2:3]
            w_bf, sg = [], []
            for part in range(2):
                w = early[part, pair] * stats[pair, part : part + 1]
                w_bf.append(w.astype(jnp.bfloat16))
                sg.append((w * (early_gw[part, pair] - row_mean)).astype(jnp.bfloat16))
            w_bf, sg = jnp.concatenate(w_bf, axis=0), jnp.concatenate(sg, axis=0)
            w_parts.append(w_bf)
            sg_parts.append(sg)
            out = dot(value_cols, jnp.concatenate([weights[pair], w_bf], axis=0))
            dq = dot(key_cols, jnp.concatenate([grads[pair], sg], axis=0)) * SCALE
            for k in range(2):
                half = slice(k * rows, (k + 1) * rows)
                att[2 * pair + k] = out[:, half].T.astype(jnp.bfloat16)
                qg[2 * pair + k] = dq[:, half].T.astype(jnp.bfloat16)
        dk = dot(jnp.concatenate(sg_parts, axis=1), all_heads(q, head)) * SCALE
        dv = dot(jnp.concatenate(w_parts, axis=1), all_heads(g, head))
        for part, grad in enumerate((dk, dv)):
            dbefore[head, part] = grad[:rows].astype(jnp.bfloat16)
            down[head, part] = grad[rows:]
        send(dbefore.at[head], after_grad.at[head], send_sems.at[6], recv_sems.at[6], trunk, previous)

        def store(i):
            at = head * 2 * per_group + i
            pltpu.make_async_copy(att.at[at], att_out.at[:, columns(at)], store_sems.at[0]).start()
            pltpu.make_async_copy(qg.at[at], qg_out.at[:, columns(at)], store_sems.at[1]).start()

        loop(0, 2 * per_group, store)

    loop(0, HEADS_BEFORE_SUMS, rest_group)

    arrived(came, recv_sems.at[5])

    all_sums = dot(
        hits[...].reshape(n_branch * piece_rows, n_served * piece_rows),
        came[...].reshape(n_served * piece_rows, DH),
    )
    summed[...] = all_sums.astype(jnp.bfloat16).reshape(summed.shape)
    to_branch(lambda b: summed.at[b], sums.at[branch], send_sems.at[7], recv_sems.at[7])

    loop(HEADS_BEFORE_SUMS, KVH, rest_group)

    arrived(after_grad, recv_sems.at[6])

    for part in range(2):
        for head in range(KVH):
            kv_grad_ref[:, part, head * DH : (head + 1) * DH] = down[head, part] + after_grad[
                head, part
            ].astype(jnp.float32)
    kv_copy = pltpu.make_async_copy(kv_grad_ref, kv_out, store_sems.at[2])
    kv_copy.start()
    arrived(sums, recv_sems.at[7])
    for head in range(KVH):
        total = sums[head].astype(jnp.float32)
        for i in range(1, n_branch // KVH):
            total = total + sums[i * KVH + head].astype(jnp.float32)
        trunk_grad_ref[:, :, head * DH : (head + 1) * DH] = total

    trunk_copy = pltpu.make_async_copy(trunk_grad_ref, trunk_out, store_sems.at[3])
    trunk_copy.start()
    others = pl.ds(0, n_served - 1)
    arrived(asked.at[others], send_sems.at[0])
    arrived(held.at[pl.ds(0, n_branch - 1)], send_sems.at[1])
    arrived(own_raw, send_sems.at[2])
    arrived(tags_ref, send_sems.at[3])
    arrived(staged.at[others], send_sems.at[4])
    arrived(came.at[others], send_sems.at[5])
    arrived(dbefore, send_sems.at[6])
    arrived(sums.at[pl.ds(0, n_branch - 1)], send_sems.at[7])
    arrived(att, store_sems.at[0])
    arrived(qg, store_sems.at[1])
    kv_copy.wait()
    trunk_copy.wait()


def fused(n_trunk, n_branch, queries, out_grad, own, segment, asked, tags, reach):
    rows, width = queries.shape
    n_served = n_trunk * KVH
    heads = width // DH
    piece = (2, segment.shape[1], DH)
    trunk_len = n_trunk * segment.shape[1]
    by_head = (KVH, 2, rows, DH)
    anywhere = pl.BlockSpec(memory_space=pl.ANY)
    bf16, f32 = jnp.bfloat16, jnp.float32
    return pl.pallas_call(
        functools.partial(kernel, n_trunk, n_branch),
        in_specs=[pl.BlockSpec(memory_space=pltpu.HBM)] * 7,
        out_specs=[anywhere] * 4,
        out_shape=[
            jax.ShapeDtypeStruct(queries.shape, bf16),
            jax.ShapeDtypeStruct(queries.shape, bf16),
            jax.ShapeDtypeStruct(own.shape, f32),
            jax.ShapeDtypeStruct(segment.shape, f32),
        ],
        scratch_shapes=[
            pltpu.VMEM((heads, rows, DH), bf16),
            pltpu.VMEM((heads, rows, DH), bf16),
            *[pltpu.VMEM(a.shape, a.dtype) for a in (own, segment, asked, tags, reach)],
            pltpu.VMEM(own.shape, f32),
            pltpu.VMEM(segment.shape, f32),
            pltpu.VMEM((n_branch, *piece), bf16),
            pltpu.VMEM((n_served, *asked.shape), jnp.int32),
            pltpu.SMEM((n_served, *asked.shape), jnp.int32),
            pltpu.VMEM((n_served, *piece), bf16),
            pltpu.VMEM((KVH, n_trunk, *piece), bf16),
            pltpu.VMEM(own.shape, bf16),
            pltpu.VMEM(by_head, bf16),
            pltpu.VMEM(by_head, bf16),
            pltpu.VMEM(tags.shape, jnp.int32),
            pltpu.VMEM((3, rows, rows), f32),
            pltpu.VMEM((2, heads // 2, rows, 2 * rows), f32),
            pltpu.VMEM((2, heads // 2, rows, 2 * rows), f32),
            pltpu.VMEM((heads // 2, 8, 2 * rows), f32),
            pltpu.VMEM((heads // 2, trunk_len, 2 * rows), bf16),
            pltpu.VMEM((heads // 2, trunk_len, 2 * rows), bf16),
            pltpu.VMEM((heads, rows, DH), bf16),
            pltpu.VMEM((heads, rows, DH), bf16),
            pltpu.VMEM((KVH, n_trunk, *piece), bf16),
            pltpu.VMEM(by_head, bf16),
            pltpu.VMEM(by_head, f32),
            pltpu.VMEM((n_served, *piece), bf16),
            pltpu.VMEM((n_branch, 2 * piece[1], n_served * 2 * piece[1]), bf16),
            pltpu.VMEM((n_branch, *piece), bf16),
            pltpu.VMEM((n_branch, *piece), bf16),
            pltpu.VMEM(by_head, bf16),
            pltpu.SemaphoreType.DMA((7,)),
            pltpu.SemaphoreType.DMA((4,)),
            pltpu.SemaphoreType.DMA,
            pltpu.SemaphoreType.DMA((8,)),
            pltpu.SemaphoreType.DMA((8,)),
        ],
        compiler_params=pltpu.CompilerParams(
            collective_id=0, has_side_effects=True, vmem_limit_bytes=40 << 20
        ),
        name="tree_attention",
    )(queries, out_grad, own, segment, asked, tags, reach)


def assemble_kernel(*refs):
    count = len(refs) // 2
    copies = [pltpu.make_async_copy(refs[i], refs[count + i], refs[-1].at[i]) for i in range(count)]
    for copy in copies:
        copy.start()
    for copy in copies:
        copy.wait()


def assemble(*arrays):
    anywhere = pl.BlockSpec(memory_space=pl.ANY)
    return pl.pallas_call(
        assemble_kernel,
        in_specs=[anywhere] * len(arrays),
        out_specs=[anywhere] * len(arrays),
        out_shape=[jax.ShapeDtypeStruct(a.shape, a.dtype) for a in arrays],
        scratch_shapes=[pltpu.SemaphoreType.DMA((len(arrays),))],
        compiler_params=pltpu.CompilerParams(vmem_limit_bytes=8 << 20),
        name="assemble",
    )(*arrays)


def on_device(queries, keys_values, out_grad, trunk_kv, branch_of, branch_reach, ancestors):
    n_trunk, n_branch = lax.axis_size("trunk"), lax.axis_size("branch")
    arrays = (queries[0], out_grad[0], keys_values[0], trunk_kv[0, 0], ancestors[0], branch_of, branch_reach)
    arrays = [pltpu.with_memory_space_constraint(a, pltpu.HBM) for a in arrays]
    results = fused(n_trunk, n_branch, *arrays)
    attended, query_grad, kv_grad, trunk_grad = assemble(*results)
    return (attended[None], query_grad[None], kv_grad[None], trunk_grad[None, None])


def solution(mesh):
    return jax.shard_map(
        on_device,
        mesh=mesh,
        in_specs=(
            P("trunk", "branch", None),
            P("trunk", "branch", None, None),
            P("trunk", "branch", None),
            P("trunk", "branch", None, None, None),
            P("trunk", "branch"),
            P("trunk", None),
            P("trunk", "branch", None),
        ),
        out_specs=(
            P("trunk", "branch", None),
            P("trunk", "branch", None),
            P("trunk", "branch", None, None),
            P("trunk", "branch", None, None, None),
        ),
        check_vma=False,
    )
```

```python
import functools
import math

import jax
import jax.numpy as jnp
from jax import lax
from jax.experimental import pallas as pl
from jax.experimental.pallas import tpu as pltpu
from jax.sharding import PartitionSpec as P

KVH = 4
DH = 128
NEG = -1e30
SCALE = 1.0 / math.sqrt(DH)
EXP2_SCALE = SCALE * math.log2(math.e)
MESH = pl.DeviceIdType.MESH
NT = (((1,), (1,)), ((), ()))
SENT_FIRST = 2


def dot(a, b):
    return jnp.dot(a, b, preferred_element_type=jnp.float32)


def dot_nt(a, b):
    return lax.dot_general(a, b, NT, preferred_element_type=jnp.float32)


def signal(semaphore, trunk, branch):
    pl.semaphore_signal(semaphore, inc=1, device_id=(trunk, branch), device_id_type=MESH)


def send(source, target, send_sem, recv_sem, trunk, branch):
    pltpu.make_async_remote_copy(
        src_ref=source,
        dst_ref=target,
        send_sem=send_sem,
        recv_sem=recv_sem,
        device_id=(trunk, branch),
        device_id_type=MESH,
    ).start()


def arrived(ref, sem):
    pltpu.make_async_copy(ref, ref, sem).wait()


def loop(first, last, body):
    def step(i, carry):
        body(i)
        return carry

    lax.fori_loop(first, last, step, 0)


def far_first(n):
    return [(n // 2 + (i + 1) // 2 * (-1 if i % 2 else 1)) % n for i in range(n)]


def columns(head):
    return pl.ds(pl.multiple_of(head * DH, DH), DH)


def split_up(raw, kv):
    for part in range(2):
        both = raw[:, part, :]
        for head in range(KVH):
            kv[head, part] = both[:, head * DH : (head + 1) * DH]


def kernel(
    n_trunk, n_branch,
    q_hbm, g_hbm, own_hbm, segment_hbm, asked_hbm, tags_hbm, reach_hbm,
    att_out, qg_out, kv_out, trunk_out,
    q, g, own_raw, segment_ref, asked_ref, tags_ref, reach_ref, kv_grad_ref, trunk_grad_ref, held, asked, wanted, staged, got, before_raw, own_ref, before, before_tags, bias, early, early_gw, stats,
    weights, grads, att, qg, dtrunk, dbefore, down, came, hits, summed, sums, after_grad,
    load_sems, store_sems, local_sem, send_sems, recv_sems, head_sems,
):
    trunk, branch = lax.axis_index("trunk"), lax.axis_index("branch")
    z, y = branch // KVH, lax.rem(branch, KVH)
    me = trunk * KVH + y
    n_served = n_trunk * KVH
    heads = q.shape[0]
    pairs = heads // 2
    per_group = pairs // KVH
    rows = q.shape[1]
    trunk_len = n_trunk * segment_ref.shape[1]
    after = lax.rem(branch + 1, n_branch)
    previous = lax.rem(branch + n_branch - 1, n_branch)

    ys = [lax.rem(y + d, KVH) for d in far_first(KVH)]
    zs = [lax.rem(z + d, n_branch // KVH) for d in far_first(n_branch // KVH)]
    ts = [lax.rem(trunk + d, n_trunk) for d in far_first(n_trunk)]
    in_branch = [at * KVH + other for at in zs for other in ys][:-1]
    in_served = [(t, other) for t in ts for other in ys][:-1]

    inputs = [
        pltpu.make_async_copy(source, target, load_sems.at[2 + i])
        for i, (source, target) in enumerate(
            (
                (asked_hbm, asked_ref),
                (segment_hbm, segment_ref),
                (own_hbm, own_raw),
                (tags_hbm, tags_ref),
                (reach_hbm, reach_ref),
            )
        )
    ]
    for copy in inputs:
        copy.start()
    barrier = pltpu.get_barrier_semaphore()
    for other in in_branch:
        signal(barrier, trunk, other)
    for t, other in in_served[: (n_trunk - 1) * KVH]:
        signal(barrier, t, z * KVH + other)
    for copy in inputs:
        copy.wait()
    pl.semaphore_wait(barrier, n_branch - 1 + (n_trunk - 1) * KVH)

    def to_served(source, target, send_sem, recv_sem):
        for t, other in in_served:
            send(source(t, other), target, send_sem, recv_sem, t, z * KVH + other)
        pltpu.make_async_copy(source(trunk, y), target, recv_sem).start()

    def to_branch(source, target, send_sem, recv_sem):
        for other in in_branch:
            send(source(other), target, send_sem, recv_sem, trunk, other)
        pltpu.make_async_copy(source(branch), target, recv_sem).start()

    to_served(lambda t, o: asked_ref, asked.at[me], send_sems.at[0], recv_sems.at[0])
    to_branch(
        lambda b: segment_ref.at[:, :, columns(lax.rem(b, KVH))],
        held.at[branch],
        send_sems.at[1],
        recv_sems.at[1],
    )
    send(own_raw, before_raw, send_sems.at[2], recv_sems.at[2], trunk, after)
    send(tags_ref, before_tags, send_sems.at[3], recv_sems.at[3], trunk, after)

    def load(i):
        pltpu.make_async_copy(q_hbm.at[:, columns(i)], q.at[i], load_sems.at[0]).start()
        pltpu.make_async_copy(g_hbm.at[:, columns(i)], g.at[i], load_sems.at[1]).start()

    loop(0, heads, load)

    split_up(own_raw, own_ref)
    squares = jnp.broadcast_to(tags_ref[...], (rows, rows))
    position = lax.broadcasted_iota(jnp.int32, (rows, rows), 0)
    query = lax.broadcasted_iota(jnp.int32, (rows, rows), 1)
    bias[2] = jnp.where((squares.T == squares) & (position <= query), 0.0, NEG)
    branches = reach_ref.shape[1]
    reach_column = jnp.broadcast_to(reach_ref[...].astype(jnp.float32), (branches, branches)).T
    branch_index = lax.broadcasted_iota(jnp.int32, (branches, rows), 0)
    reach = jnp.sum(
        jnp.where(branch_index == tags_ref[...], reach_column[:, :1], 0.0), axis=0, keepdims=True
    )
    depth = lax.broadcasted_iota(jnp.int32, (trunk_len, rows), 0) // segment_ref.shape[1]
    bias[0] = jnp.where(depth.astype(jnp.float32) < reach, 0.0, NEG)

    def two_heads(ref, pair):
        return ref[pl.ds(2 * pair, 2)].reshape(2 * rows, DH)

    def twice(part):
        return jnp.concatenate([bias[part], bias[part]], axis=1)

    def start_part(part, pair, keys, values):
        scores = dot_nt(keys, two_heads(q, pair)) + twice(part)
        highest = jnp.max(scores, axis=0, keepdims=True)
        expo = jnp.exp2((scores - highest) * EXP2_SCALE)
        gw = dot_nt(values, two_heads(g, pair))
        total = jnp.sum(expo, axis=0, keepdims=True)
        mean = jnp.sum(expo * gw, axis=0, keepdims=True)
        return expo, gw, highest, total, mean

    def start_early(part, kv):
        def group(head):
            keys, values = kv[head, 0], kv[head, 1]
            for i in range(per_group):
                pair = head * per_group + i
                expo, gw, *rest = start_part(part + 1, pair, keys, values)
                early[part, pair] = expo
                early_gw[part, pair] = gw
                for k in range(3):
                    stats[pair, 3 * part + k : 3 * part + k + 1] = rest[k]

        loop(0, KVH, group)

    arrived(q, load_sems.at[0])
    arrived(g, load_sems.at[1])
    start_early(1, own_ref)

    arrived(asked, recv_sems.at[0])
    local = pltpu.make_async_copy(asked, wanted, local_sem)
    local.start()
    local.wait()

    piece_rows = 2 * segment_ref.shape[1]
    lane = lax.broadcasted_iota(jnp.int32, (piece_rows, DH), 1)
    line = lax.broadcasted_iota(jnp.int32, (piece_rows, DH), 0)
    diagonal = jnp.where(lax.rem(lane, piece_rows) == line, 1.0, 0.0)
    per_tile = DH // piece_rows
    sources = []
    for tile in range(n_served // per_tile):
        source = jnp.full((piece_rows, DH), wanted[tile * per_tile, 0, trunk], jnp.int32)
        for i in range(1, per_tile):
            source = jnp.where(lane >= i * piece_rows, wanted[tile * per_tile + i, 0, trunk], source)
        sources.append(source)

    def mark(owner):
        for tile, source in enumerate(sources):
            hits[owner, :, tile * DH : (tile + 1) * DH] = jnp.where(source == owner, diagonal, 0.0).astype(
                jnp.bfloat16
            )

    loop(0, n_branch, mark)
    arrived(held, recv_sems.at[1])

    for i in range(n_served):
        staged[i] = held[wanted[i, 0, trunk]]
    to_served(
        lambda t, o: staged.at[t * KVH + o], got.at[y, trunk], send_sems.at[4], head_sems.at[y]
    )

    arrived(before_tags, recv_sems.at[3])
    earlier_tags = jnp.where(branch > 0, before_tags[...], -1)
    bias[1] = jnp.where(jnp.broadcast_to(earlier_tags, (rows, rows)).T == squares, 0.0, NEG)
    arrived(before_raw, recv_sems.at[2])
    split_up(before_raw, before)
    start_early(0, before)

    def fetched(head, part):
        return got[head, :, part].reshape(trunk_len, DH)

    def all_heads(ref, head):
        return ref[pl.ds(head * 2 * per_group, 2 * per_group)].reshape(2 * per_group * rows, DH)

    def trunk_group(turn):
        head = lax.rem(y + turn, KVH)
        arrived(got.at[head], head_sems.at[head])
        keys, values = fetched(head, 0), fetched(head, 1)
        known = [stats[head * per_group + i] for i in range(per_group)]
        merged, w_parts, sg_parts = [], [], []
        for i in range(per_group):
            pair = head * per_group + i
            expo, gw, highest, total, mean = start_part(0, pair, keys, values)
            peaks, totals, means = [
                [known[i][k : k + 1], known[i][k + 3 : k + 4], last]
                for k, last in enumerate((highest, total, mean))
            ]
            best = jnp.maximum(peaks[2], jnp.maximum(peaks[0], peaks[1]))
            factors = [jnp.exp2((m - best) * EXP2_SCALE) for m in peaks]
            norm = 1.0 / sum(f * t for f, t in zip(factors, totals))
            factors = [f * norm for f in factors]
            row_mean = sum(f * t for f, t in zip(factors, means))
            merged.append((factors[0], factors[1], row_mean))
            w = expo * factors[2]
            w_parts.append(w.astype(jnp.bfloat16))
            sg_parts.append((w * (gw - row_mean)).astype(jnp.bfloat16))
        dv = dot(jnp.concatenate(w_parts, axis=1), all_heads(g, head))
        dk = dot(jnp.concatenate(sg_parts, axis=1), all_heads(q, head)) * SCALE
        for part, grad in enumerate((dk, dv)):
            dtrunk[head, :, part] = grad.reshape(n_trunk, -1, DH).astype(jnp.bfloat16)

        def give(t):
            send(dtrunk.at[head, t], came.at[me], send_sems.at[5], recv_sems.at[5], t, z * KVH + head)

        for t in ts[:-1]:
            give(t)

        @pl.when(head != y)
        def _():
            give(trunk)

        @pl.when(head == y)
        def _():
            pltpu.make_async_copy(dtrunk.at[head, trunk], came.at[me], recv_sems.at[5]).start()

        for i in range(per_group):
            pair = head * per_group + i
            for k in range(3):
                stats[pair, k : k + 1] = merged[i][k]
            weights[pair, :trunk_len] = w_parts[i]
            grads[pair, :trunk_len] = sg_parts[i]

    loop(0, KVH, trunk_group)

    def final_part(part, pair):
        known = stats[pair]
        w = early[part, pair] * known[part : part + 1]
        return w.astype(jnp.bfloat16), (w * (early_gw[part, pair] - known[2:3])).astype(jnp.bfloat16)

    def key_grads(w_parts, sg_parts, head):
        dk = dot(jnp.concatenate(sg_parts, axis=1), all_heads(q, head)) * SCALE
        return dk, dot(jnp.concatenate(w_parts, axis=1), all_heads(g, head))

    def before_group(head):
        w_parts, sg_parts = zip(*[final_part(0, head * per_group + i) for i in range(per_group)])
        for part, grad in enumerate(key_grads(w_parts, sg_parts, head)):
            dbefore[head, part] = grad.astype(jnp.bfloat16)
        for i in range(per_group):
            pair = head * per_group + i
            weights[pair, trunk_len:] = w_parts[i]
            grads[pair, trunk_len:] = sg_parts[i]

    def send_before(head):
        send(dbefore.at[head], after_grad.at[head], send_sems.at[6], recv_sems.at[6], trunk, previous)

    def own_group(head):
        key_cols = jnp.concatenate([fetched(head, 0), before[head, 0], own_ref[head, 0]], axis=0).T
        value_cols = jnp.concatenate([fetched(head, 1), before[head, 1], own_ref[head, 1]], axis=0).T
        w_parts, sg_parts = zip(*[final_part(1, head * per_group + i) for i in range(per_group)])
        for i in range(per_group):
            pair = head * per_group + i
            out = dot(value_cols, jnp.concatenate([weights[pair], w_parts[i]], axis=0))
            dq = dot(key_cols, jnp.concatenate([grads[pair], sg_parts[i]], axis=0)) * SCALE
            for k in range(2):
                half = slice(k * rows, (k + 1) * rows)
                att[2 * pair + k] = out[:, half].T.astype(jnp.bfloat16)
                qg[2 * pair + k] = dq[:, half].T.astype(jnp.bfloat16)
        for part, grad in enumerate(key_grads(w_parts, sg_parts, head)):
            down[head, part] = grad

        def store(i):
            at = head * 2 * per_group + i
            pltpu.make_async_copy(att.at[at], att_out.at[:, columns(at)], store_sems.at[0]).start()
            pltpu.make_async_copy(qg.at[at], qg_out.at[:, columns(at)], store_sems.at[1]).start()

        loop(0, 2 * per_group, store)

    def before_and_send(head):
        before_group(head)
        send_before(head)

    loop(0, SENT_FIRST, before_and_send)
    loop(SENT_FIRST, KVH, before_group)

    arrived(came, recv_sems.at[5])

    all_sums = dot(
        hits[...].reshape(n_branch * piece_rows, n_served * piece_rows),
        came[...].reshape(n_served * piece_rows, DH),
    )
    summed[...] = all_sums.astype(jnp.bfloat16).reshape(summed.shape)
    to_branch(lambda b: summed.at[b], sums.at[branch], send_sems.at[7], recv_sems.at[7])

    loop(SENT_FIRST, KVH, send_before)
    loop(0, KVH, own_group)

    arrived(after_grad, recv_sems.at[6])

    for part in range(2):
        for head in range(KVH):
            kv_grad_ref[:, part, head * DH : (head + 1) * DH] = down[head, part] + after_grad[
                head, part
            ].astype(jnp.float32)
    kv_copy = pltpu.make_async_copy(kv_grad_ref, kv_out, store_sems.at[2])
    kv_copy.start()
    arrived(sums, recv_sems.at[7])
    for head in range(KVH):
        total = sums[head].astype(jnp.float32)
        for i in range(1, n_branch // KVH):
            total = total + sums[i * KVH + head].astype(jnp.float32)
        trunk_grad_ref[:, :, head * DH : (head + 1) * DH] = total

    trunk_copy = pltpu.make_async_copy(trunk_grad_ref, trunk_out, store_sems.at[3])
    trunk_copy.start()
    others = pl.ds(0, n_served - 1)
    arrived(asked.at[others], send_sems.at[0])
    arrived(held.at[pl.ds(0, n_branch - 1)], send_sems.at[1])
    arrived(own_raw, send_sems.at[2])
    arrived(tags_ref, send_sems.at[3])
    arrived(staged.at[others], send_sems.at[4])
    arrived(came.at[others], send_sems.at[5])
    arrived(dbefore, send_sems.at[6])
    arrived(sums.at[pl.ds(0, n_branch - 1)], send_sems.at[7])
    arrived(att, store_sems.at[0])
    arrived(qg, store_sems.at[1])
    kv_copy.wait()
    trunk_copy.wait()


def fused(n_trunk, n_branch, queries, out_grad, own, segment, asked, tags, reach):
    rows, width = queries.shape
    n_served = n_trunk * KVH
    heads = width // DH
    piece = (2, segment.shape[1], DH)
    trunk_len = n_trunk * segment.shape[1]
    by_head = (KVH, 2, rows, DH)
    anywhere = pl.BlockSpec(memory_space=pl.ANY)
    bf16, f32 = jnp.bfloat16, jnp.float32
    return pl.pallas_call(
        functools.partial(kernel, n_trunk, n_branch),
        in_specs=[pl.BlockSpec(memory_space=pltpu.HBM)] * 7,
        out_specs=[anywhere] * 4,
        out_shape=[
            jax.ShapeDtypeStruct(queries.shape, bf16),
            jax.ShapeDtypeStruct(queries.shape, bf16),
            jax.ShapeDtypeStruct(own.shape, f32),
            jax.ShapeDtypeStruct(segment.shape, f32),
        ],
        scratch_shapes=[
            pltpu.VMEM((heads, rows, DH), bf16),
            pltpu.VMEM((heads, rows, DH), bf16),
            *[pltpu.VMEM(a.shape, a.dtype) for a in (own, segment, asked, tags, reach)],
            pltpu.VMEM(own.shape, f32),
            pltpu.VMEM(segment.shape, f32),
            pltpu.VMEM((n_branch, *piece), bf16),
            pltpu.VMEM((n_served, *asked.shape), jnp.int32),
            pltpu.SMEM((n_served, *asked.shape), jnp.int32),
            pltpu.VMEM((n_served, *piece), bf16),
            pltpu.VMEM((KVH, n_trunk, *piece), bf16),
            pltpu.VMEM(own.shape, bf16),
            pltpu.VMEM(by_head, bf16),
            pltpu.VMEM(by_head, bf16),
            pltpu.VMEM(tags.shape, jnp.int32),
            pltpu.VMEM((3, rows, rows), f32),
            pltpu.VMEM((2, heads // 2, rows, 2 * rows), f32),
            pltpu.VMEM((2, heads // 2, rows, 2 * rows), f32),
            pltpu.VMEM((heads // 2, 8, 2 * rows), f32),
            pltpu.VMEM((heads // 2, trunk_len + rows, 2 * rows), bf16),
            pltpu.VMEM((heads // 2, trunk_len + rows, 2 * rows), bf16),
            pltpu.VMEM((heads, rows, DH), bf16),
            pltpu.VMEM((heads, rows, DH), bf16),
            pltpu.VMEM((KVH, n_trunk, *piece), bf16),
            pltpu.VMEM(by_head, bf16),
            pltpu.VMEM(by_head, f32),
            pltpu.VMEM((n_served, *piece), bf16),
            pltpu.VMEM((n_branch, 2 * piece[1], n_served * 2 * piece[1]), bf16),
            pltpu.VMEM((n_branch, *piece), bf16),
            pltpu.VMEM((n_branch, *piece), bf16),
            pltpu.VMEM(by_head, bf16),
            pltpu.SemaphoreType.DMA((7,)),
            pltpu.SemaphoreType.DMA((4,)),
            pltpu.SemaphoreType.DMA,
            pltpu.SemaphoreType.DMA((8,)),
            pltpu.SemaphoreType.DMA((8,)),
            pltpu.SemaphoreType.DMA((KVH,)),
        ],
        compiler_params=pltpu.CompilerParams(
            collective_id=0, has_side_effects=True, vmem_limit_bytes=40 << 20
        ),
        name="tree_attention",
    )(queries, out_grad, own, segment, asked, tags, reach)


def assemble_kernel(*refs):
    count = len(refs) // 2
    copies = [pltpu.make_async_copy(refs[i], refs[count + i], refs[-1].at[i]) for i in range(count)]
    for copy in copies:
        copy.start()
    for copy in copies:
        copy.wait()


def assemble(*arrays):
    anywhere = pl.BlockSpec(memory_space=pl.ANY)
    return pl.pallas_call(
        assemble_kernel,
        in_specs=[anywhere] * len(arrays),
        out_specs=[anywhere] * len(arrays),
        out_shape=[jax.ShapeDtypeStruct(a.shape, a.dtype) for a in arrays],
        scratch_shapes=[pltpu.SemaphoreType.DMA((len(arrays),))],
        compiler_params=pltpu.CompilerParams(vmem_limit_bytes=8 << 20),
        name="assemble",
    )(*arrays)


def on_device(queries, keys_values, out_grad, trunk_kv, branch_of, branch_reach, ancestors):
    n_trunk, n_branch = lax.axis_size("trunk"), lax.axis_size("branch")
    arrays = (queries[0], out_grad[0], keys_values[0], trunk_kv[0, 0], ancestors[0], branch_of, branch_reach)
    arrays = [pltpu.with_memory_space_constraint(a, pltpu.HBM) for a in arrays]
    results = fused(n_trunk, n_branch, *arrays)
    attended, query_grad, kv_grad, trunk_grad = assemble(*results)
    return (attended[None], query_grad[None], kv_grad[None], trunk_grad[None, None])


def solution(mesh):
    return jax.shard_map(
        on_device,
        mesh=mesh,
        in_specs=(
            P("trunk", "branch", None),
            P("trunk", "branch", None, None),
            P("trunk", "branch", None),
            P("trunk", "branch", None, None, None),
            P("trunk", "branch"),
            P("trunk", None),
            P("trunk", "branch", None),
        ),
        out_specs=(
            P("trunk", "branch", None),
            P("trunk", "branch", None),
            P("trunk", "branch", None, None),
            P("trunk", "branch", None, None, None),
        ),
        check_vma=False,
    )
```

```python
import functools
import math

import jax
import jax.numpy as jnp
from jax import lax
from jax.experimental import pallas as pl
from jax.experimental.pallas import tpu as pltpu
from jax.sharding import PartitionSpec as P

KVH = 4
DH = 128
NEG = -1e30
SCALE = 1.0 / math.sqrt(DH)
EXP2_SCALE = SCALE * math.log2(math.e)
MESH = pl.DeviceIdType.MESH
NT = (((1,), (1,)), ((), ()))
SENT_FIRST = 2


def dot(a, b):
    return jnp.dot(a, b, preferred_element_type=jnp.float32)


def dot_nt(a, b):
    return lax.dot_general(a, b, NT, preferred_element_type=jnp.float32)


def signal(semaphore, trunk, branch):
    pl.semaphore_signal(semaphore, inc=1, device_id=(trunk, branch), device_id_type=MESH)


def send(source, target, send_sem, recv_sem, trunk, branch):
    pltpu.make_async_remote_copy(
        src_ref=source,
        dst_ref=target,
        send_sem=send_sem,
        recv_sem=recv_sem,
        device_id=(trunk, branch),
        device_id_type=MESH,
    ).start()


def arrived(ref, sem):
    pltpu.make_async_copy(ref, ref, sem).wait()


def loop(first, last, body):
    def step(i, carry):
        body(i)
        return carry

    lax.fori_loop(first, last, step, 0)


def far_first(n):
    return [(n // 2 + (i + 1) // 2 * (-1 if i % 2 else 1)) % n for i in range(n)]


def columns(head):
    return pl.ds(pl.multiple_of(head * DH, DH), DH)


def split_up(raw, kv):
    for part in range(2):
        both = raw[:, part, :]
        for head in range(KVH):
            kv[head, part] = both[:, head * DH : (head + 1) * DH]


def kernel(
    n_trunk, n_branch,
    q_hbm, g_hbm, own_hbm, segment_hbm, asked_hbm, tags_hbm, reach_hbm,
    att_out, qg_out, kv_out, trunk_out,
    q, g, own_raw, segment_ref, asked_ref, tags_ref, reach_ref, kv_grad_ref, trunk_grad_ref, held, asked, wanted, staged, got, before_raw, own_ref, before, before_tags, bias, early, early_gw, stats,
    weights, grads, att, qg, dtrunk, dbefore, down, came, hits, summed, sums, after_grad,
    load_sems, store_sems, local_sem, send_sems, recv_sems, head_sems,
):
    trunk, branch = lax.axis_index("trunk"), lax.axis_index("branch")
    z, y = branch // KVH, lax.rem(branch, KVH)
    me = trunk * KVH + y
    n_served = n_trunk * KVH
    heads = q.shape[0]
    pairs = heads // 2
    per_group = pairs // KVH
    rows = q.shape[1]
    trunk_len = n_trunk * segment_ref.shape[1]
    after = lax.rem(branch + 1, n_branch)
    previous = lax.rem(branch + n_branch - 1, n_branch)

    ys = [lax.rem(y + d, KVH) for d in far_first(KVH)]
    zs = [lax.rem(z + d, n_branch // KVH) for d in far_first(n_branch // KVH)]
    ts = [lax.rem(trunk + d, n_trunk) for d in far_first(n_trunk)]
    in_branch = [at * KVH + other for at in zs for other in ys][:-1]
    in_served = [(t, other) for t in ts for other in ys][:-1]

    inputs = [
        pltpu.make_async_copy(source, target, load_sems.at[2 + i])
        for i, (source, target) in enumerate(
            (
                (asked_hbm, asked_ref),
                (segment_hbm, segment_ref),
                (own_hbm, own_raw),
                (tags_hbm, tags_ref),
                (reach_hbm, reach_ref),
            )
        )
    ]
    for copy in inputs:
        copy.start()
    barrier = pltpu.get_barrier_semaphore()
    for other in in_branch:
        signal(barrier, trunk, other)
    for t, other in in_served[: (n_trunk - 1) * KVH]:
        signal(barrier, t, z * KVH + other)
    for copy in inputs:
        copy.wait()
    pl.semaphore_wait(barrier, n_branch - 1 + (n_trunk - 1) * KVH)

    def to_served(source, target, send_sem, recv_sem):
        for t, other in in_served:
            send(source(t, other), target, send_sem, recv_sem, t, z * KVH + other)
        pltpu.make_async_copy(source(trunk, y), target, recv_sem).start()

    def to_branch(source, target, send_sem, recv_sem):
        for other in in_branch:
            send(source(other), target, send_sem, recv_sem, trunk, other)
        pltpu.make_async_copy(source(branch), target, recv_sem).start()

    to_branch(
        lambda b: segment_ref.at[:, :, columns(lax.rem(b, KVH))],
        held.at[branch],
        send_sems.at[1],
        recv_sems.at[1],
    )
    to_served(lambda t, o: asked_ref, asked.at[me], send_sems.at[0], recv_sems.at[0])
    send(own_raw, before_raw, send_sems.at[2], recv_sems.at[2], trunk, after)
    send(tags_ref, before_tags, send_sems.at[3], recv_sems.at[3], trunk, after)

    def load(i):
        pltpu.make_async_copy(q_hbm.at[:, columns(i)], q.at[i], load_sems.at[0]).start()
        pltpu.make_async_copy(g_hbm.at[:, columns(i)], g.at[i], load_sems.at[1]).start()

    loop(0, heads, load)

    split_up(own_raw, own_ref)
    squares = jnp.broadcast_to(tags_ref[...], (rows, rows))
    position = lax.broadcasted_iota(jnp.int32, (rows, rows), 0)
    query = lax.broadcasted_iota(jnp.int32, (rows, rows), 1)
    bias[2] = jnp.where((squares.T == squares) & (position <= query), 0.0, NEG)
    branches = reach_ref.shape[1]
    reach_column = jnp.broadcast_to(reach_ref[...].astype(jnp.float32), (branches, branches)).T
    branch_index = lax.broadcasted_iota(jnp.int32, (branches, rows), 0)
    reach = jnp.sum(
        jnp.where(branch_index == tags_ref[...], reach_column[:, :1], 0.0), axis=0, keepdims=True
    )
    depth = lax.broadcasted_iota(jnp.int32, (trunk_len, rows), 0) // segment_ref.shape[1]
    bias[0] = jnp.where(depth.astype(jnp.float32) < reach, 0.0, NEG)

    def two_heads(ref, pair):
        return ref[pl.ds(2 * pair, 2)].reshape(2 * rows, DH)

    def twice(part):
        return jnp.concatenate([bias[part], bias[part]], axis=1)

    def start_part(part, pair, keys, values):
        scores = dot_nt(keys, two_heads(q, pair)) + twice(part)
        highest = jnp.max(scores, axis=0, keepdims=True)
        expo = jnp.exp2((scores - highest) * EXP2_SCALE)
        gw = dot_nt(values, two_heads(g, pair))
        total = jnp.sum(expo, axis=0, keepdims=True)
        mean = jnp.sum(expo * gw, axis=0, keepdims=True)
        return expo, gw, highest, total, mean

    def start_early(part, kv):
        def group(head):
            keys, values = kv[head, 0], kv[head, 1]
            for i in range(per_group):
                pair = head * per_group + i
                expo, gw, *rest = start_part(part + 1, pair, keys, values)
                early[part, pair] = expo
                early_gw[part, pair] = gw
                for k in range(3):
                    stats[pair, 3 * part + k : 3 * part + k + 1] = rest[k]

        loop(0, KVH, group)

    arrived(q, load_sems.at[0])
    arrived(g, load_sems.at[1])
    start_early(1, own_ref)

    arrived(asked, recv_sems.at[0])
    local = pltpu.make_async_copy(asked, wanted, local_sem)
    local.start()
    local.wait()

    piece_rows = 2 * segment_ref.shape[1]
    lane = lax.broadcasted_iota(jnp.int32, (piece_rows, DH), 1)
    line = lax.broadcasted_iota(jnp.int32, (piece_rows, DH), 0)
    diagonal = jnp.where(lax.rem(lane, piece_rows) == line, 1.0, 0.0)
    per_tile = DH // piece_rows
    sources = []
    for tile in range(n_served // per_tile):
        source = jnp.full((piece_rows, DH), wanted[tile * per_tile, 0, trunk], jnp.int32)
        for i in range(1, per_tile):
            source = jnp.where(lane >= i * piece_rows, wanted[tile * per_tile + i, 0, trunk], source)
        sources.append(source)

    def mark(owner):
        for tile, source in enumerate(sources):
            hits[owner, :, tile * DH : (tile + 1) * DH] = jnp.where(source == owner, diagonal, 0.0).astype(
                jnp.bfloat16
            )

    loop(0, n_branch, mark)
    arrived(held, recv_sems.at[1])

    for i in range(n_served):
        staged[i] = held[wanted[i, 0, trunk]]
    to_served(
        lambda t, o: staged.at[t * KVH + o], got.at[y, trunk], send_sems.at[4], head_sems.at[y]
    )

    arrived(before_tags, recv_sems.at[3])
    earlier_tags = jnp.where(branch > 0, before_tags[...], -1)
    bias[1] = jnp.where(jnp.broadcast_to(earlier_tags, (rows, rows)).T == squares, 0.0, NEG)
    arrived(before_raw, recv_sems.at[2])
    split_up(before_raw, before)
    start_early(0, before)

    def fetched(head, part):
        return got[head, :, part].reshape(trunk_len, DH)

    def all_heads(ref, head):
        return ref[pl.ds(head * 2 * per_group, 2 * per_group)].reshape(2 * per_group * rows, DH)

    def trunk_group(turn):
        head = lax.rem(y + turn, KVH)
        arrived(got.at[head], head_sems.at[head])
        keys, values = fetched(head, 0), fetched(head, 1)
        known = [stats[head * per_group + i] for i in range(per_group)]
        merged, w_parts, sg_parts = [], [], []
        for i in range(per_group):
            pair = head * per_group + i
            expo, gw, highest, total, mean = start_part(0, pair, keys, values)
            peaks, totals, means = [
                [known[i][k : k + 1], known[i][k + 3 : k + 4], last]
                for k, last in enumerate((highest, total, mean))
            ]
            best = jnp.maximum(peaks[2], jnp.maximum(peaks[0], peaks[1]))
            factors = [jnp.exp2((m - best) * EXP2_SCALE) for m in peaks]
            norm = 1.0 / sum(f * t for f, t in zip(factors, totals))
            factors = [f * norm for f in factors]
            row_mean = sum(f * t for f, t in zip(factors, means))
            merged.append((factors[0], factors[1], row_mean))
            w = expo * factors[2]
            w_parts.append(w.astype(jnp.bfloat16))
            sg_parts.append((w * (gw - row_mean)).astype(jnp.bfloat16))
        dv = dot(jnp.concatenate(w_parts, axis=1), all_heads(g, head))
        dk = dot(jnp.concatenate(sg_parts, axis=1), all_heads(q, head)) * SCALE
        for part, grad in enumerate((dk, dv)):
            dtrunk[head, :, part] = grad.reshape(n_trunk, -1, DH).astype(jnp.bfloat16)

        def give(t):
            send(dtrunk.at[head, t], came.at[me], send_sems.at[5], recv_sems.at[5], t, z * KVH + head)

        for t in ts[:-1]:
            give(t)

        @pl.when(head != y)
        def _():
            give(trunk)

        @pl.when(head == y)
        def _():
            pltpu.make_async_copy(dtrunk.at[head, trunk], came.at[me], recv_sems.at[5]).start()

        for i in range(per_group):
            pair = head * per_group + i
            for k in range(3):
                stats[pair, k : k + 1] = merged[i][k]
            weights[pair, :trunk_len] = w_parts[i]
            grads[pair, :trunk_len] = sg_parts[i]

    loop(0, KVH, trunk_group)

    def final_part(part, pair):
        known = stats[pair]
        w = early[part, pair] * known[part : part + 1]
        return w.astype(jnp.bfloat16), (w * (early_gw[part, pair] - known[2:3])).astype(jnp.bfloat16)

    def key_grads(w_parts, sg_parts, head):
        dk = dot(jnp.concatenate(sg_parts, axis=1), all_heads(q, head)) * SCALE
        return dk, dot(jnp.concatenate(w_parts, axis=1), all_heads(g, head))

    def before_group(head):
        w_parts, sg_parts = zip(*[final_part(0, head * per_group + i) for i in range(per_group)])
        for part, grad in enumerate(key_grads(w_parts, sg_parts, head)):
            dbefore[head, part] = grad.astype(jnp.bfloat16)
        for i in range(per_group):
            pair = head * per_group + i
            weights[pair, trunk_len:] = w_parts[i]
            grads[pair, trunk_len:] = sg_parts[i]

    def send_before(head):
        send(dbefore.at[head], after_grad.at[head], send_sems.at[6], recv_sems.at[6], trunk, previous)

    def own_group(head):
        key_cols = jnp.concatenate([fetched(head, 0), before[head, 0], own_ref[head, 0]], axis=0).T
        value_cols = jnp.concatenate([fetched(head, 1), before[head, 1], own_ref[head, 1]], axis=0).T
        w_parts, sg_parts = zip(*[final_part(1, head * per_group + i) for i in range(per_group)])
        for i in range(per_group):
            pair = head * per_group + i
            out = dot(value_cols, jnp.concatenate([weights[pair], w_parts[i]], axis=0))
            dq = dot(key_cols, jnp.concatenate([grads[pair], sg_parts[i]], axis=0)) * SCALE
            for k in range(2):
                half = slice(k * rows, (k + 1) * rows)
                att[2 * pair + k] = out[:, half].T.astype(jnp.bfloat16)
                qg[2 * pair + k] = dq[:, half].T.astype(jnp.bfloat16)
        for part, grad in enumerate(key_grads(w_parts, sg_parts, head)):
            down[head, part] = grad

        def store(i):
            at = head * 2 * per_group + i
            pltpu.make_async_copy(att.at[at], att_out.at[:, columns(at)], store_sems.at[0]).start()
            pltpu.make_async_copy(qg.at[at], qg_out.at[:, columns(at)], store_sems.at[1]).start()

        loop(0, 2 * per_group, store)

    def before_and_send(head):
        before_group(head)
        send_before(head)

    loop(0, SENT_FIRST, before_and_send)
    loop(SENT_FIRST, KVH, before_group)

    arrived(came, recv_sems.at[5])

    arrivals = came[...].reshape(n_served * piece_rows, DH)
    half = len(zs) // 2
    for k in range(2):
        mine = zs[k * half : (k + 1) * half]
        marks = [hits[pl.ds(at * KVH, KVH)].reshape(KVH * piece_rows, -1) for at in mine]
        part = dot(jnp.concatenate(marks, axis=0), arrivals).astype(jnp.bfloat16)
        part = part.reshape(half, KVH, *summed.shape[1:])
        for i, at in enumerate(mine):
            summed[pl.ds(at * KVH, KVH)] = part[i]
        for other in in_branch[k * half * KVH : (k + 1) * half * KVH]:
            send(summed.at[other], sums.at[branch], send_sems.at[7], recv_sems.at[7], trunk, other)
    pltpu.make_async_copy(summed.at[branch], sums.at[branch], recv_sems.at[7]).start()

    loop(SENT_FIRST, KVH, send_before)
    loop(0, KVH, own_group)

    arrived(after_grad, recv_sems.at[6])

    for part in range(2):
        for head in range(KVH):
            kv_grad_ref[:, part, head * DH : (head + 1) * DH] = down[head, part] + after_grad[
                head, part
            ].astype(jnp.float32)
    kv_copy = pltpu.make_async_copy(kv_grad_ref, kv_out, store_sems.at[2])
    kv_copy.start()
    arrived(sums, recv_sems.at[7])
    for head in range(KVH):
        total = sums[head].astype(jnp.float32)
        for i in range(1, n_branch // KVH):
            total = total + sums[i * KVH + head].astype(jnp.float32)
        trunk_grad_ref[:, :, head * DH : (head + 1) * DH] = total

    trunk_copy = pltpu.make_async_copy(trunk_grad_ref, trunk_out, store_sems.at[3])
    trunk_copy.start()
    others = pl.ds(0, n_served - 1)
    arrived(asked.at[others], send_sems.at[0])
    arrived(held.at[pl.ds(0, n_branch - 1)], send_sems.at[1])
    arrived(own_raw, send_sems.at[2])
    arrived(tags_ref, send_sems.at[3])
    arrived(staged.at[others], send_sems.at[4])
    arrived(came.at[others], send_sems.at[5])
    arrived(dbefore, send_sems.at[6])
    arrived(sums.at[pl.ds(0, n_branch - 1)], send_sems.at[7])
    arrived(att, store_sems.at[0])
    arrived(qg, store_sems.at[1])
    kv_copy.wait()
    trunk_copy.wait()


def fused(n_trunk, n_branch, queries, out_grad, own, segment, asked, tags, reach):
    rows, width = queries.shape
    n_served = n_trunk * KVH
    heads = width // DH
    piece = (2, segment.shape[1], DH)
    trunk_len = n_trunk * segment.shape[1]
    by_head = (KVH, 2, rows, DH)
    anywhere = pl.BlockSpec(memory_space=pl.ANY)
    bf16, f32 = jnp.bfloat16, jnp.float32
    return pl.pallas_call(
        functools.partial(kernel, n_trunk, n_branch),
        in_specs=[pl.BlockSpec(memory_space=pltpu.HBM)] * 7,
        out_specs=[anywhere] * 4,
        out_shape=[
            jax.ShapeDtypeStruct(queries.shape, bf16),
            jax.ShapeDtypeStruct(queries.shape, bf16),
            jax.ShapeDtypeStruct(own.shape, f32),
            jax.ShapeDtypeStruct(segment.shape, f32),
        ],
        scratch_shapes=[
            pltpu.VMEM((heads, rows, DH), bf16),
            pltpu.VMEM((heads, rows, DH), bf16),
            *[pltpu.VMEM(a.shape, a.dtype) for a in (own, segment, asked, tags, reach)],
            pltpu.VMEM(own.shape, f32),
            pltpu.VMEM(segment.shape, f32),
            pltpu.VMEM((n_branch, *piece), bf16),
            pltpu.VMEM((n_served, *asked.shape), jnp.int32),
            pltpu.SMEM((n_served, *asked.shape), jnp.int32),
            pltpu.VMEM((n_served, *piece), bf16),
            pltpu.VMEM((KVH, n_trunk, *piece), bf16),
            pltpu.VMEM(own.shape, bf16),
            pltpu.VMEM(by_head, bf16),
            pltpu.VMEM(by_head, bf16),
            pltpu.VMEM(tags.shape, jnp.int32),
            pltpu.VMEM((3, rows, rows), f32),
            pltpu.VMEM((2, heads // 2, rows, 2 * rows), f32),
            pltpu.VMEM((2, heads // 2, rows, 2 * rows), f32),
            pltpu.VMEM((heads // 2, 8, 2 * rows), f32),
            pltpu.VMEM((heads // 2, trunk_len + rows, 2 * rows), bf16),
            pltpu.VMEM((heads // 2, trunk_len + rows, 2 * rows), bf16),
            pltpu.VMEM((heads, rows, DH), bf16),
            pltpu.VMEM((heads, rows, DH), bf16),
            pltpu.VMEM((KVH, n_trunk, *piece), bf16),
            pltpu.VMEM(by_head, bf16),
            pltpu.VMEM(by_head, f32),
            pltpu.VMEM((n_served, *piece), bf16),
            pltpu.VMEM((n_branch, 2 * piece[1], n_served * 2 * piece[1]), bf16),
            pltpu.VMEM((n_branch, *piece), bf16),
            pltpu.VMEM((n_branch, *piece), bf16),
            pltpu.VMEM(by_head, bf16),
            pltpu.SemaphoreType.DMA((7,)),
            pltpu.SemaphoreType.DMA((4,)),
            pltpu.SemaphoreType.DMA,
            pltpu.SemaphoreType.DMA((8,)),
            pltpu.SemaphoreType.DMA((8,)),
            pltpu.SemaphoreType.DMA((KVH,)),
        ],
        compiler_params=pltpu.CompilerParams(
            collective_id=0, has_side_effects=True, vmem_limit_bytes=40 << 20
        ),
        name="tree_attention",
    )(queries, out_grad, own, segment, asked, tags, reach)


def assemble_kernel(*refs):
    count = len(refs) // 2
    copies = []
    for i in range(count):
        source, target = refs[i], refs[count + i]
        step = source.shape[0] // 2
        for k in range(2):
            at = pl.ds(k * step, step)
            copies.append(pltpu.make_async_copy(source.at[at], target.at[at], refs[-1].at[i, k]))
    for copy in copies:
        copy.start()
    for copy in copies:
        copy.wait()


def assemble(*arrays):
    anywhere = pl.BlockSpec(memory_space=pl.ANY)
    return pl.pallas_call(
        assemble_kernel,
        in_specs=[anywhere] * len(arrays),
        out_specs=[anywhere] * len(arrays),
        out_shape=[jax.ShapeDtypeStruct(a.shape, a.dtype) for a in arrays],
        scratch_shapes=[pltpu.SemaphoreType.DMA((len(arrays), 2))],
        compiler_params=pltpu.CompilerParams(vmem_limit_bytes=8 << 20),
        name="assemble",
    )(*arrays)


def on_device(queries, keys_values, out_grad, trunk_kv, branch_of, branch_reach, ancestors):
    n_trunk, n_branch = lax.axis_size("trunk"), lax.axis_size("branch")
    arrays = (queries[0], out_grad[0], keys_values[0], trunk_kv[0, 0], ancestors[0], branch_of, branch_reach)
    arrays = [pltpu.with_memory_space_constraint(a, pltpu.HBM) for a in arrays]
    results = fused(n_trunk, n_branch, *arrays)
    attended, query_grad, kv_grad, trunk_grad = assemble(*results)
    return (attended[None], query_grad[None], kv_grad[None], trunk_grad[None, None])


def solution(mesh):
    return jax.shard_map(
        on_device,
        mesh=mesh,
        in_specs=(
            P("trunk", "branch", None),
            P("trunk", "branch", None, None),
            P("trunk", "branch", None),
            P("trunk", "branch", None, None, None),
            P("trunk", "branch"),
            P("trunk", None),
            P("trunk", "branch", None),
        ),
        out_specs=(
            P("trunk", "branch", None),
            P("trunk", "branch", None),
            P("trunk", "branch", None, None),
            P("trunk", "branch", None, None, None),
        ),
        check_vma=False,
    )
```
